32 devices in a mesh: dp: 8 (over z, y), rows: 4 (over x, core).
Axes of the slice: x: 2, y: 2, z: 4, core: 2. Of those that a mesh axis runs over, the one named last changes fastest.
Arguments:
- real_frames: bfloat16 [8, 3, 64, 256], P('dp', None, 'rows'), may hold values from -4 to 4
- fake_frames: bfloat16 [8, 3, 64, 256], P('dp', None, 'rows'), may hold values from -4 to 4
- conv_one: bfloat16 [3, 3, 3, 64], replicated, may hold values from -1.25 to 1.25
- conv_two: bfloat16 [3, 3, 64, 128], replicated, may hold values from -0.25 to 0.25
- conv_three: bfloat16 [3, 3, 128, 256], replicated, may hold values from -0.1875 to 0.1875
- conv_four: bfloat16 [3, 3, 256, 512], replicated, may hold values from -0.125 to 0.125
- conv_five: bfloat16 [3, 3, 512, 512], replicated, may hold values from -0.09375 to 0.09375
- bias_one: float32 [64], replicated, may hold values from -2 to 2
- bias_two: float32 [128], replicated, may hold values from -2 to 2
- bias_three: float32 [256], replicated, may hold values from -2 to 2
- bias_four: float32 [512], replicated, may hold values from -2 to 2
- bias_five: float32 [512], replicated, may hold values from -2 to 2
- linear_one: float32 [64], replicated, may hold values from 0.05 to 2
- linear_two: float32 [128], replicated, may hold values from 0.05 to 2
- linear_three: float32 [256], replicated, may hold values from 0.05 to 2
- linear_four: float32 [512], replicated, may hold values from 0.05 to 2
- linear_five: float32 [512], replicated, may hold values from 0.25 to 10
Outputs:
- tap_losses: float32 [5], replicated
- fake_grad: float32 [8, 3, 64, 256], P('dp', None, 'rows')
The draws below stay inside these ranges and needn't reach their ends.
All inputs are finite; a program needn't handle non-finite values.
Results may differ from the reference program's by a relative error of at most 0.0065.
Values may be sent and summed in bfloat16 or wider, within the bound.
No kernel may reach another device: no remote copies, remote signals or barrier semaphores. Data moves between devices by JAX's collectives and lax.ppermute only.
A program may use at most 128 MiB of HBM per device.

```python
import math
import jax
import jax.numpy as jnp
from jax import lax

C1 = 64
C2 = 128
C3 = 256
C4 = 512
C5 = 512
WIDTH = 256
FRAMES = 8
HEIGHT = 64


def coarse_field(key):
    small = jax.random.normal(key, (FRAMES, 3, HEIGHT // 16, WIDTH // 16), jnp.float32)
    return jnp.repeat(jnp.repeat(small, 16, axis=2), 16, axis=3)


def frame_pair(key):
    base = jax.random.fold_in(key, 4711)
    keys = jax.random.split(base, 4)
    rough_real = jax.random.normal(keys[0], (FRAMES, 3, HEIGHT, WIDTH), jnp.float32)
    rough_diff = jax.random.normal(keys[1], (FRAMES, 3, HEIGHT, WIDTH), jnp.float32)
    coarse_real = coarse_field(keys[2])
    coarse_diff = coarse_field(keys[3])
    place = jnp.arange(FRAMES, dtype=jnp.float32) / max(FRAMES - 1, 1)
    rise = 0.3 + 0.7 * place
    real = 0.5 * rough_real + 0.8 * coarse_real
    fake = real + rise[:, None, None, None] * (0.4 * rough_diff + 0.8 * coarse_diff)
    return (jnp.clip(real, -4.0, 4.0), jnp.clip(fake, -4.0, 4.0))


def draw_real_frames(key, part):
    return frame_pair(key)[0].astype(jnp.bfloat16)


def draw_fake_frames(key, part):
    return frame_pair(key)[1].astype(jnp.bfloat16)


def noise(own_key, dims, spread, reach, kind=jnp.bfloat16):
    array = spread * jax.random.normal(own_key, dims, jnp.float32)
    return jnp.clip(array, min=-reach, max=reach).astype(kind)


def setup_inputs(seed: int = 0) -> dict:
    key_of = jax.random.split(jax.random.key(seed), 18)
    real_frames = draw_real_frames(jax.random.fold_in(key_of[17], 71), 0)
    fake_frames = draw_fake_frames(jax.random.fold_in(key_of[17], 71), 0)
    conv_one = noise(key_of[2], (3, 3, 3, C1), 27 ** -0.5, 1.25)
    conv_two = noise(key_of[3], (3, 3, C1, C2), (9 * C1) ** -0.5, 0.25)
    conv_three = noise(key_of[4], (3, 3, C2, C3), (9 * C2) ** -0.5, 0.1875)
    conv_four = noise(key_of[5], (3, 3, C3, C4), (9 * C3) ** -0.5, 0.125)
    conv_five = noise(key_of[6], (3, 3, C4, C5), (9 * C4) ** -0.5, 0.09375)
    bias_one = noise(key_of[7], (C1,), 0.5, 2.0, jnp.float32)
    bias_two = noise(key_of[8], (C2,), 0.5, 2.0, jnp.float32)
    bias_three = noise(key_of[9], (C3,), 0.5, 2.0, jnp.float32)
    bias_four = noise(key_of[10], (C4,), 0.5, 2.0, jnp.float32)
    bias_five = noise(key_of[11], (C5,), 0.5, 2.0, jnp.float32)
    linear_one = jnp.clip(jnp.exp(jax.random.uniform(key_of[12], (C1,), jnp.float32, math.log(0.05), math.log(2.0))), 0.05, 2.0)
    linear_two = jnp.clip(jnp.exp(jax.random.uniform(key_of[13], (C2,), jnp.float32, math.log(0.05), math.log(2.0))), 0.05, 2.0)
    linear_three = jnp.clip(jnp.exp(jax.random.uniform(key_of[14], (C3,), jnp.float32, math.log(0.05), math.log(2.0))), 0.05, 2.0)
    linear_four = jnp.clip(jnp.exp(jax.random.uniform(key_of[15], (C4,), jnp.float32, math.log(0.05), math.log(2.0))), 0.05, 2.0)
    linear_five = jnp.clip(jnp.exp(jax.random.uniform(key_of[16], (C5,), jnp.float32, math.log(0.25), math.log(10.0))), 0.25, 10.0)
    return {"real_frames": real_frames, "fake_frames": fake_frames, "conv_one": conv_one, "conv_two": conv_two, "conv_three": conv_three, "conv_four": conv_four, "conv_five": conv_five, "bias_one": bias_one, "bias_two": bias_two, "bias_three": bias_three, "bias_four": bias_four, "bias_five": bias_five, "linear_one": linear_one, "linear_two": linear_two, "linear_three": linear_three, "linear_four": linear_four, "linear_five": linear_five}


EPS = 1e-06

def smooth(values):
    return jax.nn.gelu(values, approximate=True)

def smooth_back(pre_act, grad_out):
    _, pullback = jax.vjp(smooth, pre_act)
    return pullback(grad_out)[0]

def conv_same(inputs, kernel):
    return lax.conv_general_dilated(inputs.astype(jnp.float32), kernel.astype(jnp.float32), (1, 1), ((1, 1), (1, 1)), dimension_numbers=('NHWC', 'HWIO', 'NHWC'), precision=lax.Precision.HIGHEST)

def flipped(kernel):
    return jnp.transpose(jnp.flip(kernel, (0, 1)), (0, 1, 3, 2))

def pool_half(values):
    shaped = values.astype(jnp.float32).reshape(values.shape[0], values.shape[1] // 2, 2, values.shape[2] // 2, 2, values.shape[3])
    return lax.optimization_barrier(jnp.mean(shaped, axis=(2, 4))).astype(jnp.bfloat16)

def unpool_half(values):
    return jnp.repeat(jnp.repeat(values, 2, axis=1), 2, axis=2) * 0.25

def tap_terms(real_feat, fake_feat, linear):
    real_float = real_feat.astype(jnp.float32)
    fake_float = fake_feat.astype(jnp.float32)
    real_norm = jnp.sqrt(lax.optimization_barrier(jnp.sum(real_float * real_float, axis=-1, keepdims=True)) + EPS)
    fake_norm = jnp.sqrt(lax.optimization_barrier(jnp.sum(fake_float * fake_float, axis=-1, keepdims=True)) + EPS)
    real_unit = real_float / real_norm
    fake_unit = fake_float / fake_norm
    differ = real_unit - fake_unit
    tap_map = lax.optimization_barrier(jnp.sum(linear * differ * differ, axis=-1))
    upward = -2.0 * linear * differ
    tap_grad = (upward - fake_unit * lax.optimization_barrier(jnp.sum(fake_unit * upward, axis=-1, keepdims=True))) / fake_norm
    return (tap_map, tap_grad)

def one_frame(pair, kernels, biases, linears):
    real_frame, fake_frame = pair
    inputs = jnp.transpose(jnp.stack([real_frame, fake_frame]), (0, 2, 3, 1))
    stored = []
    values = []
    for segment_no in range(5):
        pre_act = conv_same(inputs, kernels[segment_no]) + biases[segment_no]
        post_act = smooth(pre_act).astype(jnp.bfloat16)
        tap_map, tap_grad = tap_terms(post_act[0:1], post_act[1:2], linears[segment_no])
        values.append(jnp.mean(tap_map))
        stored.append((pre_act[1:2], tap_grad))
        if segment_no < 4:
            inputs = pool_half(post_act)
    grad_input = None
    for segment_no in range(4, -1, -1):
        pre_fake, tap_grad = stored[segment_no]
        grad_act = tap_grad * 4.0 ** segment_no
        if grad_input is not None:
            grad_act = grad_act + unpool_half(grad_input)
        grad_pre = smooth_back(pre_fake, grad_act).astype(jnp.bfloat16)
        grad_input = conv_same(grad_pre, flipped(kernels[segment_no]))
    return (jnp.stack(values), jnp.transpose(grad_input[0], (2, 0, 1)))

def reference(real_frames, fake_frames, conv_one, conv_two, conv_three, conv_four, conv_five, bias_one, bias_two, bias_three, bias_four, bias_five, linear_one, linear_two, linear_three, linear_four, linear_five):
    kernels = (conv_one, conv_two, conv_three, conv_four, conv_five)
    biases = (bias_one, bias_two, bias_three, bias_four, bias_five)
    linears = (linear_one, linear_two, linear_three, linear_four, linear_five)

    def per_frame(pair):
        return one_frame(pair, kernels, biases, linears)
    values, grads = lax.map(per_frame, (real_frames, fake_frames))
    return (lax.optimization_barrier(jnp.mean(values, axis=0)), grads)
```

```python
import functools
import math

import jax
import jax.numpy as jnp
from jax import lax
from jax.experimental import pallas as pl
from jax.experimental.pallas import tpu as pltpu
from jax.sharding import PartitionSpec as P

EPS = 1e-06
F32 = jnp.float32
BF16 = jnp.bfloat16
K0 = math.sqrt(2.0 / math.pi)
K1 = K0 * 0.044715
PH = 16
LANES = 128
HALF = 64


def gelu(x):
    return x * (0.5 + 0.5 * jnp.tanh(x * (K0 + K1 * (x * x))))


def gelu_back(x):
    sq = x * x
    t = jnp.tanh(x * (K0 + K1 * sq))
    return (0.5 + 0.5 * t) + (x * (1.0 - t * t)) * (0.5 * K0 + (1.5 * K1) * sq)


def dot(a, b):
    return lax.dot_general(a, b, (((1,), (0,)), ((), ())), preferred_element_type=F32)


def dot_t(a, b):
    return lax.dot_general(a, b, (((1,), (1,)), ((), ())), preferred_element_type=F32)


def iota(shape, dim):
    return lax.broadcasted_iota(jnp.int32, shape, dim)


def low_half(shape):
    return iota(shape, len(shape) - 1) % LANES < HALF


def shifted(value, step):
    n, length, chans = value.shape
    flat = value.reshape(n * length, chans)
    place = iota(flat.shape, 0) % length
    if step > 0:
        out = jnp.where(place == 0, 0.0, pltpu.roll(flat, 1, 0))
    else:
        out = jnp.where(place == length - 1, 0.0, pltpu.roll(flat, n * length - 1, 0))
    return out.reshape(n, length, chans)


def prep_body(real_ref, fake_ref, out_ref):
    _, rows, width = real_ref.shape
    length = width // PH
    shape = (rows * length, width)
    col = iota(shape, 1)
    place = iota(shape, 0) % length
    inside = col // PH == place
    edges = (col == place * PH - 1) | (col == place * PH + PH)
    eshape = (width, LANES)
    ecol = iota(eshape, 0) % PH
    lane = iota(eshape, 1)
    total = jnp.zeros((rows * length, LANES), F32)
    for img, ref in enumerate((real_ref, fake_ref)):
        for ch in range(3):
            x = ref[ch].astype(F32)
            wide = jnp.broadcast_to(x[:, None, :], (rows, length, width)).reshape(shape)
            base = img * HALF + ch
            a = jnp.concatenate(
                [jnp.where(inside, wide, 0.0), jnp.where(edges, wide, 0.0)], axis=1
            ).astype(BF16)
            e_in = lane == base + (ecol + 1) * 3
            e_edge = ((ecol == PH - 1) & (lane == base)) | (
                (ecol == 0) & (lane == base + (PH + 1) * 3)
            )
            e = jnp.concatenate(
                [jnp.where(e_in, 1.0, 0.0), jnp.where(e_edge, 1.0, 0.0)], axis=0
            ).astype(BF16)
            total = total + dot(a, e)
    out_ref[...] = total.astype(BF16).reshape(rows, length, LANES)


def prep(real, fake):
    _, rows, width = real.shape
    return pl.pallas_call(
        prep_body,
        out_shape=jax.ShapeDtypeStruct((rows, width // PH, LANES), BF16),
        name="prep",
    )(real, fake)


def main_body(
    dims,
    x_ref, c1_ref, c2_ref, w3_hbm, w4_hbm, w5_hbm,
    b1_ref, b2_ref, b3_ref, b4_ref, b5_ref,
    l1_ref, l2_ref, l3_ref, l4_ref, l5_ref,
    loss_ref, grad_ref,
    w3, w4, w5, sems, base, w1, r1, w2, w2t,
    rowv, xk,
    p1, p2, p3, p4,
    a1, a2, a3, a4, a5, z1, z2, z3, z4, z5,
    g1, g2, g3, g4, g5, i2, i3, i4, i5,
):
    H, L, HB, C1, C2, C3, C4, C5 = dims
    band = lax.axis_index("rows")
    copies = [
        pltpu.make_async_copy(src, dst, sems.at[i])
        for i, (src, dst) in enumerate(((w3_hbm, w3), (w4_hbm, w4), (w5_hbm, w5)))
    ]
    for copy in copies:
        copy.start()

    base[...] = jnp.zeros(base.shape, F32)
    for dr in range(3):
        for dc in range(3):
            blk = c1_ref[dr, dc].astype(F32)
            base[dr, dc * 3 : dc * 3 + 3, 0:HALF] = blk
            base[dr, dc * 3 : dc * 3 + 3, HALF:LANES] = blk
    rows64 = base.shape[1]
    lo = low_half((rows64, LANES))
    for dr in range(3):
        b = base[dr]
        for i in range(PH // 2):
            first = pltpu.roll(b, (6 * i) % rows64, 0) if i else b
            blk = jnp.where(lo, first, pltpu.roll(b, (6 * i + 3) % rows64, 0))
            w1[dr * HALF : (dr + 1) * HALF, i * LANES : (i + 1) * LANES] = blk.astype(BF16)
        b = base[2 - dr]
        for j in range(PH // 2 + 2):
            s0, s1 = ((6 * j - 9) % rows64, (6 * j - 6) % rows64)
            blk = jnp.where(
                lo,
                pltpu.roll(b, s0, 0) if s0 else b,
                pltpu.roll(b, s1, 0) if s1 else b,
            )
            k = (dr * (PH // 2 + 2) + j) * LANES
            r1[:, k : k + LANES] = blk.astype(BF16)
    w1[3 * HALF : 4 * HALF, :] = jnp.zeros((HALF, w1.shape[1]), BF16)
    w2[...] = jnp.zeros(w2.shape, BF16)
    w2t[...] = jnp.zeros(w2t.shape, BF16)
    for dr in range(3):
        for dc in range(3):
            blk = c2_ref[dr * 3 + dc]
            k = (dr * 3 + dc) * 2 * C1
            w2[k : k + C1, 0:C2] = blk
            w2[k + C1 : k + 2 * C1, C2 : 2 * C2] = blk
            back = c2_ref[(2 - dr) * 3 + 2 - dc]
            for u in range(2):
                k = (dr * 4 + dc + u) * C2
                for d in range(2):
                    n = (u * 2 + d) * C1
                    w2t[n : n + C1, k : k + C2] = back
    for s, (b_ref, l_ref) in enumerate(
        ((b1_ref, l1_ref), (b2_ref, l2_ref), (b3_ref, l3_ref), (b4_ref, l4_ref), (b5_ref, l5_ref))
    ):
        wide = b_ref.shape[1]
        rowv[s : s + 1, 0:wide] = b_ref[...]
        rowv[8 + s : 9 + s, 0:wide] = l_ref[...]
        if s < 2:
            rowv[s : s + 1, wide : 2 * wide] = b_ref[...]
        if s < 1:
            rowv[8 + s : 9 + s, wide : 2 * wide] = l_ref[...]

    for p in (p1, p2):
        n = p.shape[0]
        p[0] = jnp.zeros(p.shape[1:], BF16)
        p[n - 1] = jnp.zeros(p.shape[1:], BF16)
    for p in (p3, p4):
        n = p.shape[1]
        for img in range(2):
            p[img, 0] = jnp.zeros(p.shape[2:], BF16)
            p[img, n - 1] = jnp.zeros(p.shape[2:], BF16)

    x = x_ref[...].astype(F32)
    xr = pltpu.roll(x.reshape(H * L, LANES), HALF, 1).reshape(H, L, LANES)
    zero = jnp.zeros((1, L, LANES), F32)
    lo3 = low_half((H, L, LANES))

    def above(v):
        return jnp.concatenate([zero, v[: H - 1]], axis=0)

    def below(v):
        return jnp.concatenate([v[1:], zero], axis=0)

    xk[0, :, :, 0:LANES] = jnp.where(lo3, above(x), xr).astype(BF16)
    xk[0, :, :, LANES : 2 * LANES] = below(x).astype(BF16)
    xk[1, :, :, 0:LANES] = jnp.where(lo3, above(xr), x).astype(BF16)
    xk[1, :, :, LANES : 2 * LANES] = below(xr).astype(BF16)

    rows = 8

    @pl.loop(0, H // rows)
    def _(step):
        r0 = step * rows
        lop = low_half((rows // 2, L, LANES))
        bias = jnp.concatenate([rowv[0:1, 0:LANES]] * 2, axis=1)
        for n in range(PH // 4):
            sums = []
            for img in range(2):
                lhs = xk[img, pl.ds(r0, rows)].reshape(rows * L, 2 * LANES)
                z = dot(lhs, w1[:, n * 256 : (n + 1) * 256]) + bias
                act = gelu(z)
                halves = []
                for i in range(2):
                    part = act[:, i * LANES : (i + 1) * LANES].reshape(rows, L, LANES)
                    a1[img, pl.ds(r0 + 2, rows), n * 2 + i] = part.astype(BF16)
                    if img:
                        z1[pl.ds(r0 + 2, rows), n * 2 + i] = z[
                            :, i * LANES : (i + 1) * LANES
                        ].reshape(rows, L, LANES)
                    pair = part.reshape(rows // 2, 2, L, LANES)
                    halves.append(pair[:, 0] + pair[:, 1])
                sums.append(halves)
            for i in range(2):
                sr, sf = (sums[0][i], sums[1][i])
                mixed = jnp.where(lop, sf, sr).reshape(rows // 2 * L, LANES)
                mixed = pltpu.roll(mixed, HALF, 1).reshape(rows // 2, L, LANES)
                pooled = (jnp.where(lop, sr, sf) + mixed) * 0.25
                phase = n * 2 + i
                at = pl.ds(r0 // 2 + 1, rows // 2)
                p1[at, phase + 1] = pooled.astype(BF16)
                if phase == PH // 2 - 1:
                    p1[at, 0] = shifted(pooled, 1).astype(BF16)
                if phase == 0:
                    p1[at, PH // 2 + 1] = shifted(pooled, -1).astype(BF16)

    rows2 = 2
    ph2 = PH // 2

    @pl.loop(0, H // 2 // rows2)
    def _(step):
        r0 = step * rows2
        lhs = jnp.concatenate(
            [
                p1[pl.ds(r0 + dr, rows2), dc : dc + ph2].reshape(rows2 * ph2 * L, 2 * C1)
                for dr in range(3)
                for dc in range(3)
            ],
            axis=1,
        )
        z = dot(lhs, w2[...]) + rowv[1:2, 0 : 2 * C2]
        act = gelu(z)
        at = pl.ds(r0 + 2, rows2)
        for img in range(2):
            a2[img, at] = act[:, img * C2 : (img + 1) * C2].astype(BF16).reshape(rows2, ph2, L, C2)
        z2[at] = z[:, C2:].reshape(rows2, ph2, L, C2)
        pair = act.reshape(2, ph2 // 2, 2, L, 2 * C2)
        pooled = ((pair[0, :, 0] + pair[0, :, 1]) + (pair[1, :, 0] + pair[1, :, 1])) * 0.25
        row = r0 // 2 + 1
        p2[row, 1 : ph2 // 2 + 1] = pooled.astype(BF16)
        p2[row, 0] = shifted(pooled[ph2 // 2 - 1 :], 1)[0].astype(BF16)
        p2[row, ph2 // 2 + 1] = shifted(pooled[0:1], -1)[0].astype(BF16)

    copies[0].wait()
    rows3 = 4
    ph3 = PH // 4

    @pl.loop(0, H // 4 // rows3)
    def _(step):
        r0 = step * rows3
        for img in range(2):
            lhs = jnp.concatenate(
                [
                    p2[
                        pl.ds(r0 + dr, rows3), dc : dc + ph3, :, img * C2 : (img + 1) * C2
                    ].reshape(rows3 * ph3 * L, C2)
                    for dr in range(3)
                    for dc in range(3)
                ],
                axis=1,
            )
            z = dot(lhs, w3[...]) + rowv[2:3, 0:C3]
            act = gelu(z)
            at = pl.ds(r0 + 2, rows3)
            a3[img, at] = act.astype(BF16).reshape(rows3, ph3, L, C3)
            if img:
                z3[at] = z.reshape(rows3, ph3, L, C3)
            pair = act.reshape(rows3 // 2, 2, ph3 // 2, 2, L, C3)
            pooled = (
                (pair[:, 0, :, 0] + pair[:, 0, :, 1]) + (pair[:, 1, :, 0] + pair[:, 1, :, 1])
            ) * 0.25
            at = pl.ds(r0 // 2 + 1, rows3 // 2)
            p3[img, at, 1 : ph3 // 2 + 1] = pooled.astype(BF16)
            p3[img, at, 0] = shifted(pooled[:, ph3 // 2 - 1], 1).astype(BF16)
            p3[img, at, ph3 // 2 + 1] = shifted(pooled[:, 0], -1).astype(BF16)

    copies[1].wait()
    rows4 = 4
    ph4 = PH // 8

    @pl.loop(0, H // 8 // rows4)
    def _(step):
        r0 = step * rows4
        for img in range(2):
            lhs = jnp.concatenate(
                [
                    p3[img, pl.ds(r0 + dr, rows4), dc : dc + ph4].reshape(rows4 * ph4 * L, C3)
                    for dr in range(3)
                    for dc in range(3)
                ],
                axis=1,
            )
            z = dot(lhs, w4[...]) + rowv[3:4, 0:C4]
            act = gelu(z)
            at = pl.ds(r0 + 2, rows4)
            a4[img, at] = act.astype(BF16).reshape(rows4, ph4, L, C4)
            if img:
                z4[at] = z.reshape(rows4, ph4, L, C4)
            pair = act.reshape(rows4 // 2, 2, 2, L, C4)
            pooled = ((pair[:, 0, 0] + pair[:, 0, 1]) + (pair[:, 1, 0] + pair[:, 1, 1])) * 0.25
            at = pl.ds(r0 // 2 + 1, rows4 // 2)
            p4[img, at, 1] = pooled.astype(BF16)
            p4[img, at, 0] = shifted(pooled, 1).astype(BF16)
            p4[img, at, 2] = shifted(pooled, -1).astype(BF16)

    copies[2].wait()
    h5 = H // 16
    lhs = jnp.concatenate(
        [
            jnp.concatenate(
                [p4[img, dr : dr + h5, dc].reshape(h5 * L, C4) for dr in range(3) for dc in range(3)],
                axis=1,
            )
            for img in range(2)
        ],
        axis=0,
    )
    z = dot(lhs, w5[...]) + rowv[4:5, 0:C5]
    act = gelu(z).astype(BF16)
    for img in range(2):
        a5[img, 2 : 2 + h5, 0] = act[img * h5 * L : (img + 1) * h5 * L].reshape(h5, L, C5)
    z5[2 : 2 + h5, 0] = z[h5 * L :].reshape(h5, L, C5)

    loss_ref[...] = jnp.zeros(loss_ref.shape, F32)

    def taps(seg, acts, pres, grads, up, halo, chunk):
        chans = acts.shape[-1]
        phases = acts.shape[2]
        own = HB >> (seg - 1)
        total_rows = H >> (seg - 1)
        start = band * own - halo
        scale = -2.0 * 4.0 ** (seg - 1)
        count = own + 2 * halo
        ones_rows = min(chans, 256)
        group = HALF if chans == LANES and seg == 1 else ones_rows
        if seg == 1:
            width = LANES
            rr = iota((2 * LANES, 2 * LANES), 0)
            cc = iota((2 * LANES, 2 * LANES), 1)
            ones2 = jnp.where(rr // HALF == cc // HALF, 1.0, 0.0).astype(BF16)
            ones1 = ones2[0:LANES, 0:LANES]
        else:
            width = LANES
            rr = iota((2 * chans, 2 * LANES), 0)
            cc = iota((2 * chans, 2 * LANES), 1)
            ones2 = jnp.where(rr // chans == cc // LANES, 1.0, 0.0).astype(BF16)
            ones1 = jnp.ones((chans, LANES), BF16)
        reps = chans // LANES
        lin = rowv[7 + seg : 8 + seg, 0:chans]

        def spread(v):
            return jnp.concatenate([v] * reps, axis=1) if reps > 1 else v

        def piece(k):
            i0 = k * chunk
            at = pl.ds(start + i0 + 2, chunk)
            m = chunk * phases * L
            r = acts[0, at].reshape(m, chans).astype(F32)
            f = acts[1, at].reshape(m, chans).astype(F32)
            sums = dot(jnp.concatenate([r * r, f * f], axis=1).astype(BF16), ones2)
            inv_r = spread(lax.rsqrt(sums[:, 0:width] + EPS))
            inv_f = spread(lax.rsqrt(sums[:, width : 2 * width] + EPS))
            nf = f * inv_f
            d = r * inv_r - nf
            ld = lin * d
            q = spread(dot((nf * ld).astype(BF16), ones1))
            rowid = iota((chunk, phases, L, chans), 0)
            mapped = (ld * d).reshape(chunk, phases, L, chans)
            first, last = (halo - i0, halo + own - i0)
            mapped = jnp.where((rowid >= first) & (rowid < last), mapped, 0.0)
            tap = (ld - nf * q) * (inv_f * scale)
            if up is not None:
                tap = tap + up(i0, chunk).reshape(m, chans)
            g = gelu_back(pres[at].reshape(m, chans)) * tap
            g = g.reshape(chunk, phases, L, chans)
            place = rowid + (start + i0)
            g = jnp.where((place >= 0) & (place < total_rows), g, 0.0)
            to = pl.ds(i0, chunk)
            grads[to, 1 : phases + 1] = g.astype(BF16)
            grads[to, 0] = shifted(g[:, phases - 1], 1).astype(BF16)
            grads[to, phases + 1] = shifted(g[:, 0], -1).astype(BF16)
            part = jnp.sum(mapped.reshape(m, chans), axis=0, keepdims=True)
            acc = part[:, 0:LANES]
            for j in range(1, reps):
                acc = acc + part[:, j * LANES : (j + 1) * LANES]
            loss_ref[seg - 1 : seg, :] += acc

        if count == chunk:
            piece(0)
        else:
            pl.loop(0, count // chunk)(piece)

    def upper(ref, halo):
        def load(i0, chunk):
            if halo == 2:
                v = ref[pl.ds(i0 // 2, chunk // 2)]
                n, ph, length, chans = v.shape
                v = jnp.broadcast_to(v[:, None, :, None], (n, 2, ph, 2, length, chans))
                return v.reshape(2 * n, 2 * ph, length, chans)
            v = ref[pl.ds(i0 // 2, chunk // 2 + 1)]
            return jnp.stack([v[(j + 1) // 2] for j in range(chunk)])

        return load

    taps(5, a5, z5, g5, None, 2, HB // 16 + 4)
    n5 = HB // 16 + 2
    lhs = jnp.concatenate(
        [g5[dr : dr + n5, dc].reshape(n5 * L, C5) for dr in range(3) for dc in range(3)], axis=1
    )
    rhs = jnp.concatenate([w5[t * C4 : (t + 1) * C4, :] for t in range(8, -1, -1)], axis=1)
    i5[...] = (dot_t(lhs, rhs) * 0.25).reshape(n5, 1, L, C4)

    taps(4, a4, z4, g4, upper(i5, 2), 2, 2)
    n4 = HB // 8 + 2
    lhs = jnp.concatenate(
        [g4[dr : dr + n4, dc : dc + ph4].reshape(n4 * ph4 * L, C4) for dr in range(3) for dc in range(3)],
        axis=1,
    )
    rhs = jnp.concatenate([w4[t * C3 : (t + 1) * C3, :] for t in range(8, -1, -1)], axis=1)
    i4[...] = (dot_t(lhs, rhs) * 0.25).reshape(n4, ph4, L, C3)

    taps(3, a3, z3, g3, upper(i4, 2), 2, 4)
    n3 = HB // 4 + 2
    rhs = jnp.concatenate([w3[t * C2 : (t + 1) * C2, :] for t in range(8, -1, -1)], axis=1)
    lhs = jnp.concatenate(
        [g3[dr : dr + n3, dc : dc + ph3].reshape(n3 * ph3 * L, C3) for dr in range(3) for dc in range(3)],
        axis=1,
    )
    i3[...] = (dot_t(lhs, rhs) * 0.25).reshape(n3, ph3, L, C2)

    taps(2, a2, z2, g2, upper(i3, 2), 2, 4)
    n2 = HB // 2 + 2
    rowsb = 2

    @pl.loop(0, n2 // rowsb)
    def _(step):
        r0 = step * rowsb
        parts = []
        for dr in range(3):
            for j in range(4):
                v = g2[pl.ds(r0 + dr, rowsb), j : j + ph2 - 1]
                v = jnp.stack([v[:, 2 * t] for t in range(ph2 // 2)], axis=1)
                parts.append(v.reshape(rowsb * ph2 // 2 * L, C2))
        out = dot_t(jnp.concatenate(parts, axis=1), w2t[...]) * 0.25
        out = out.reshape(rowsb, ph2 // 2, L, 2 * LANES)
        both = jnp.stack([out[..., 0:LANES], out[..., LANES : 2 * LANES]], axis=2)
        i2[pl.ds(r0, rowsb)] = both.reshape(rowsb, ph2, L, LANES)

    taps(1, a1, z1, g1, upper(i2, 1), 1, 6)
    lhs = jnp.concatenate(
        [g1[dr : dr + HB, j].reshape(HB * L, LANES) for dr in range(3) for j in range(PH // 2 + 2)],
        axis=1,
    )
    gin = dot_t(lhs, r1[...])
    high = gin.astype(BF16)
    split = jnp.concatenate([high.astype(F32), gin - high.astype(F32)], axis=1).astype(BF16)
    width = PH * L
    sel_row = iota((LANES, width), 0) % HALF
    sel_col = iota((LANES, width), 1) % PH
    shape = (HB * L, width)
    inside = iota(shape, 1) // PH == iota(shape, 0) % L
    for ch in range(3):
        pick = jnp.where(sel_row == sel_col * 3 + ch, 1.0, 0.0).astype(BF16)
        spreadv = jnp.where(inside, dot(split, pick), 0.0)
        grad_ref[ch] = jnp.sum(spreadv.reshape(HB, L, width), axis=1)


def main_call(x, convs, biases, linears, band_rows):
    H, L, _ = x.shape
    HB = band_rows
    C1, C2, C3, C4, C5 = [c.shape[-1] for c in convs]
    dims = (H, L, HB, C1, C2, C3, C4, C5)
    hbm = pl.BlockSpec(memory_space=pl.ANY)
    vm = pl.BlockSpec(memory_space=pltpu.VMEM)
    ph2, ph3, ph4 = (PH // 2, PH // 4, PH // 8)
    V = pltpu.VMEM
    scratch = [
        V((9 * C2, C3), BF16), V((9 * C3, C4), BF16), V((9 * C4, C5), BF16),
        pltpu.SemaphoreType.DMA((3,)),
        V((3, HALF, LANES), F32), V((4 * HALF, PH * HALF), BF16),
        V((HALF, 3 * (ph2 + 2) * LANES), BF16), V((9 * 2 * C1, 2 * C2), BF16),
        V((4 * C1, 12 * C2), BF16),
        V((16, max(C4, C5)), F32), V((2, H, L, 2 * LANES), BF16),
        V((H // 2 + 2, ph2 + 2, L, 2 * C1), BF16), V((H // 4 + 2, ph3 + 2, L, 2 * C2), BF16),
        V((2, H // 8 + 2, ph4 + 2, L, C3), BF16), V((2, H // 16 + 2, 3, L, C4), BF16),
    ]
    acts = ((H, ph2, LANES), (H // 2, ph2, C2), (H // 4, ph3, C3), (H // 8, ph4, C4), (H // 16, 1, C5))
    scratch += [V((2, r + 4, p, L, c), BF16) for r, p, c in acts]
    scratch += [V((r + 4, p, L, c), F32) for r, p, c in acts]
    halos = (2, 4, 4, 4, 4)
    scratch += [
        V(((HB >> s) + halos[s], p + 2, L, c), BF16) for s, (_, p, c) in enumerate(acts)
    ]
    scratch += [
        V((HB // 2 + 2, ph2, L, LANES), F32), V((HB // 4 + 2, ph3, L, C2), F32),
        V((HB // 8 + 2, ph4, L, C3), F32), V((HB // 16 + 2, 1, L, C4), F32),
    ]
    c1 = convs[0]
    c2 = convs[1].reshape(9, C1, C2)
    flat = [c.reshape(-1, c.shape[-1]) for c in convs[2:]]
    vecs = [v.reshape(1, -1) for v in (*biases, *linears)]
    return pl.pallas_call(
        functools.partial(main_body, dims),
        out_shape=(
            jax.ShapeDtypeStruct((8, LANES), F32),
            jax.ShapeDtypeStruct((3, HB, L * PH), F32),
        ),
        in_specs=[vm, vm, vm, hbm, hbm, hbm] + [vm] * 10,
        out_specs=(vm, vm),
        scratch_shapes=scratch,
        name="lpips",
        compiler_params=pltpu.CompilerParams(vmem_limit_bytes=60000 * 1024),
    )(x, c1, c2, *flat, *vecs)


def summed(value):
    for axis in ("rows", "dp"):
        size = lax.axis_size(axis)
        step = 1
        while step < size:
            value = value + lax.ppermute(value, axis, [(i, i ^ step) for i in range(size)])
            step *= 2
    return value


def on_device(real_frames, fake_frames, *params):
    convs, biases, linears = (params[0:5], params[5:10], params[10:15])
    frames, _, band_rows, width = real_frames.shape
    bands = lax.axis_size("rows")
    frame_total = frames * lax.axis_size("dp")
    sums, grads = ([], [])
    for n in range(frames):
        x = prep(real_frames[n], fake_frames[n])
        x = lax.all_gather(x, "rows", axis=0, tiled=True)
        part, grad = main_call(x, convs, biases, linears, band_rows)
        sums.append(part)
        grads.append(grad)
    total = summed(functools.reduce(jnp.add, sums))
    counts = [frame_total * (band_rows * bands >> s) * (width >> s) for s in range(5)]
    losses = jnp.sum(total, axis=1)[0:5] * jnp.array([1.0 / c for c in counts], F32)
    return (losses, jnp.stack(grads))


def solution(mesh):
    frame = P("dp", None, "rows", None)
    return jax.shard_map(
        on_device,
        mesh=mesh,
        in_specs=(frame, frame) + (P(),) * 15,
        out_specs=(P(), frame),
        check_vma=False,
    )
```

```python
import functools
import math

import jax
import jax.numpy as jnp
from jax import lax
from jax.experimental import pallas as pl
from jax.experimental.pallas import tpu as pltpu
from jax.sharding import PartitionSpec as P

EPS = 1e-06
F32 = jnp.float32
BF16 = jnp.bfloat16
K0 = math.sqrt(2.0 / math.pi)
K1 = K0 * 0.044715
PH = 16
LANES = 128
HALF = 64
ONE = (PH + 2) * 3
MIB = 1 << 20
VM = pl.BlockSpec(memory_space=pltpu.VMEM)
HBM = pl.BlockSpec(memory_space=pltpu.HBM)


def gelu(h):
    t = jnp.tanh(h * (2.0 * K0 + (8.0 * K1) * (h * h)))
    return h + h * t


def gelu_back(h):
    sq = h * h
    t = jnp.tanh(h * (2.0 * K0 + (8.0 * K1) * sq))
    return (0.5 + 0.5 * t) + (h * (1.0 - t * t)) * (K0 + (12.0 * K1) * sq)


def dot(a, b):
    return lax.dot_general(a, b, (((1,), (0,)), ((), ())), preferred_element_type=F32)


def dot_t(a, b):
    return lax.dot_general(a, b, (((1,), (1,)), ((), ())), preferred_element_type=F32)


def iota(shape, dim):
    return lax.broadcasted_iota(jnp.int32, shape, dim)


def low_half(shape):
    return iota(shape, len(shape) - 1) % LANES < HALF


def shifted(value, step):
    n, length, chans = value.shape
    flat = value.reshape(n * length, chans)
    place = iota(flat.shape, 0) % length
    if step > 0:
        out = jnp.where(place == 0, 0.0, pltpu.roll(flat, 1, 0))
    else:
        out = jnp.where(place == length - 1, 0.0, pltpu.roll(flat, n * length - 1, 0))
    return out.reshape(n, length, chans)


def call(body, outs, ins, name, scratch=(), limit=16, flops=0, far=()):
    far = [pltpu.with_memory_space_constraint(v, pltpu.HBM) for v in far]
    return pl.pallas_call(
        body,
        out_shape=outs,
        in_specs=[HBM] * len(far) + [VM] * len(ins),
        out_specs=jax.tree.map(lambda _: VM, outs),
        scratch_shapes=scratch,
        name=name,
        cost_estimate=pl.CostEstimate(flops=flops, transcendentals=0, bytes_accessed=0),
        compiler_params=pltpu.CompilerParams(vmem_limit_bytes=limit * MIB),
    )(*far, *ins)


def prep_body(
    real_hbm, fake_hbm, c1_hbm, c2_hbm, b1_hbm,
    out_ref, c1, c2, b1, real_ref, fake_ref, sems,
):
    pairs = ((real_hbm, real_ref), (fake_hbm, fake_ref), (c1_hbm, c1), (c2_hbm, c2), (b1_hbm, b1))
    copies = [pltpu.make_async_copy(a, b, sems.at[i]) for i, (a, b) in enumerate(pairs)]
    for copy in copies:
        copy.start()
    _, rows, width = real_ref.shape
    length = width // PH
    shape = (rows * length, width)
    col = iota(shape, 1)
    place = iota(shape, 0) % length
    inside = col // PH == place
    edges = (col == place * PH - 1) | (col == place * PH + PH)
    eshape = (width, LANES)
    ecol = iota(eshape, 0) % PH
    lane = iota(eshape, 1)
    total = jnp.zeros((rows * length, LANES), F32)
    for copy in copies:
        copy.wait()
    for img, ref in enumerate((real_ref, fake_ref)):
        for ch in range(3):
            x = ref[ch].astype(F32)
            wide = jnp.broadcast_to(x[:, None, :], (rows, length, width)).reshape(shape)
            base = img * HALF + ch
            a = jnp.concatenate(
                [jnp.where(inside, wide, 0.0), jnp.where(edges, wide, 0.0)], axis=1
            ).astype(BF16)
            e_in = lane == base + (ecol + 1) * 3
            e_edge = ((ecol == PH - 1) & (lane == base)) | (
                (ecol == 0) & (lane == base + (PH + 1) * 3)
            )
            e = jnp.concatenate(
                [jnp.where(e_in, 1.0, 0.0), jnp.where(e_edge, 1.0, 0.0)], axis=0
            ).astype(BF16)
            total = total + dot(a, e)
    lane = iota(total.shape, 1) % HALF
    total = jnp.where((lane >= ONE) & (lane < ONE + 3), 1.0, total)
    out_ref[...] = total.astype(BF16).reshape(rows, length, LANES)


def prep(real, fake, c1, c2, b1):
    _, rows, width = real.shape
    V = pltpu.VMEM
    return call(
        prep_body,
        (V((rows, width // PH, LANES), BF16), V(c1.shape, BF16), V(c2.shape, BF16), V(b1.shape, F32)),
        (),
        "prep",
        (V(real.shape, BF16), V(fake.shape, BF16), pltpu.SemaphoreType.DMA((5,))),
        limit=8,
        far=(real, fake, c1, c2, b1),
    )


def weights_body(c1_ref, c2_ref, b1_ref, w1, r1, w2, w2t, base, bias):
    C1, C2 = c2_ref.shape[1:]
    base[...] = jnp.zeros(base.shape, F32)
    for dr in range(3):
        for dc in range(3):
            blk = c1_ref[dr, dc].astype(F32)
            base[dr, dc * 3 : dc * 3 + 3, 0:HALF] = blk
            base[dr, dc * 3 : dc * 3 + 3, HALF:LANES] = blk
    bias[0:1, 0:HALF] = b1_ref[...]
    bias[0:1, HALF:LANES] = b1_ref[...]
    left = bias[0:1, :]
    shape = (HALF, LANES)
    row = iota(shape, 0)
    lo = low_half(shape)
    extra = jnp.zeros(shape, F32)
    for k in range(3):
        part = left.astype(BF16).astype(F32)
        extra = jnp.where(row == ONE + k, jnp.broadcast_to(part, shape), extra)
        left = left - part
    for dr in range(3):
        b = base[dr]
        for i in range(PH // 2):
            first = pltpu.roll(b, (6 * i) % HALF, 0) if i else b
            blk = jnp.where(lo, first, pltpu.roll(b, (6 * i + 3) % HALF, 0))
            if dr == 1:
                blk = blk + extra
            w1[dr * HALF : (dr + 1) * HALF, i * LANES : (i + 1) * LANES] = (0.5 * blk).astype(BF16)
        b = base[2 - dr]
        for j in range(PH // 2 + 2):
            s0, s1 = ((6 * j - 9) % HALF, (6 * j - 6) % HALF)
            blk = jnp.where(
                lo, pltpu.roll(b, s0, 0) if s0 else b, pltpu.roll(b, s1, 0) if s1 else b
            )
            k = (dr * (PH // 2 + 2) + j) * LANES
            r1[:, k : k + LANES] = blk.astype(BF16)
    w1[3 * HALF : 4 * HALF, :] = jnp.zeros((HALF, w1.shape[1]), BF16)
    w2[...] = jnp.zeros(w2.shape, BF16)
    w2t[...] = jnp.zeros(w2t.shape, BF16)
    slot = (2, 0, 1, 3)
    for dr in range(3):
        for dc in range(3):
            blk = c2_ref[dr * 3 + dc]
            back = c2_ref[(2 - dr) * 3 + 2 - dc]
            for u in range(2):
                k = (dr * 4 + slot[dc + u]) * C1
                w2[k : k + C1, u * C2 : (u + 1) * C2] = blk
                k = (dr * 4 + dc + u) * C2
                for d in range(2):
                    n = (u * 2 + d) * C1
                    w2t[n : n + C1, k : k + C2] = back


def three(load):
    return jnp.concatenate([load(dr, dc) for dr in range(3) for dc in range(3)], axis=1)


def pooled_into(ref, img, row, value):
    rows, phases = value.shape[0:2]
    at = pl.ds(row + 1, rows)
    ref[img, at, 1 : phases + 1] = value.astype(BF16)
    ref[img, at, 0] = shifted(value[:, phases - 1], 1).astype(BF16)
    ref[img, at, phases + 1] = shifted(value[:, 0], -1).astype(BF16)


def inverse_norms(r, f, ones2, chans):
    sums = dot(jnp.concatenate([r * r, f * f], axis=1).astype(BF16), ones2)
    reps = chans // LANES

    def spread(v):
        return jnp.concatenate([v] * reps, axis=1) if reps > 1 else v

    inv = lax.rsqrt(sums + EPS)
    return spread(inv[:, 0:LANES]), spread(inv[:, LANES : 2 * LANES])


def ones_for(seg, chans):
    rr = iota((2 * chans, 2 * LANES), 0)
    cc = iota((2 * chans, 2 * LANES), 1)
    if seg == 1:
        return jnp.where(rr // HALF == cc // HALF, 1.0, 0.0).astype(BF16)
    return jnp.where(rr // chans == cc // LANES, 1.0, 0.0).astype(BF16)


def forward_body(
    dims,
    *refs,
):
    far, refs = (refs[0:12], refs[12:])
    x_ref, w1, w2, loss_ref, a1, a2, a3, a4, a5, z1, z2, z3, z4, z5 = refs[0:14]
    near, refs = (refs[14:26], refs[26:])
    w3, w4, w5, b2_ref, b3_ref, b4_ref, b5_ref, l1_ref, l2_ref, l3_ref, l4_ref, l5_ref = near
    xk, p1, p2, p3, p4, sems = refs
    copies = [pltpu.make_async_copy(a, b, sems.at[i]) for i, (a, b) in enumerate(zip(far, near))]
    for copy in copies[3:] + copies[:3]:
        copy.start()
    H, L, HB, C1, C2, C3, C4, C5 = dims
    ph2, ph3, ph4 = (PH // 2, PH // 4, PH // 8)
    band = lax.axis_index("rows")
    for p in (p1, p2, p3, p4):
        n = p.shape[1]
        for img in range(2):
            p[img, 0] = jnp.zeros(p.shape[2:], BF16)
            p[img, n - 1] = jnp.zeros(p.shape[2:], BF16)

    x = x_ref[...].astype(F32)
    xr = pltpu.roll(x.reshape(H * L, LANES), HALF, 1).reshape(H, L, LANES)
    zero = jnp.zeros((1, L, LANES), F32)
    lo3 = low_half((H, L, LANES))

    def above(v):
        return jnp.concatenate([zero, v[: H - 1]], axis=0)

    def below(v):
        return jnp.concatenate([v[1:], zero], axis=0)

    xk[0, :, :, 0:LANES] = jnp.where(lo3, above(x), xr).astype(BF16)
    xk[0, :, :, LANES : 2 * LANES] = below(x).astype(BF16)
    xk[1, :, :, 0:LANES] = jnp.where(lo3, above(xr), x).astype(BF16)
    xk[1, :, :, LANES : 2 * LANES] = below(xr).astype(BF16)

    def keep(r0, rows, size, first):
        place = r0 - first
        return pl.ds(jnp.where((place >= 0) & (place < size), place, size), rows)

    rows = ROWS1

    @pl.loop(0, H // rows)
    def _(step):
        r0 = step * rows
        kept = keep(r0, rows, HB + 2 * rows, band * HB - rows)
        at = pl.ds(r0 // 2 + 1, rows // 2)
        for img in range(2):
            lhs = xk[img, pl.ds(r0, rows)].reshape(rows * L, 2 * LANES)
            for n in range(PH // 4):
                h = dot(lhs, w1[:, n * 256 : (n + 1) * 256])
                act = gelu(h)
                for i in range(2):
                    lanes = slice(i * LANES, (i + 1) * LANES)
                    part = act[:, lanes].reshape(rows, L, LANES)
                    a1[img, kept, n * 2 + i] = part.astype(BF16)
                    if img:
                        z1[kept, n * 2 + i] = h[:, lanes].reshape(rows, L, LANES)
                    pair = part.reshape(rows // 2, 2, L, LANES)
                    s = (pair[:, 0] + pair[:, 1]).reshape(rows // 2 * L, LANES)
                    s = ((s + pltpu.roll(s, HALF, 1)) * 0.125).reshape(rows // 2, L, LANES)
                    half = slice(i * HALF, (i + 1) * HALF)
                    p1[img, at, n, :, half] = s.astype(BF16)[..., half]
                    q = n * 2 + i
                    other = slice((1 - i) * HALF, (2 - i) * HALF)
                    if q == ph2 - 1:
                        s = shifted(s, 1)
                    if q == 0:
                        s = shifted(s, -1)
                    slot = ph3 + (n + 1 if i else n - 1) % ph3
                    p1[img, at, slot, :, other] = s.astype(BF16)[..., other]

    for copy in copies[3:]:
        copy.wait()

    rows2 = ROWS2
    bias = jnp.concatenate([b2_ref[...]] * 2, axis=1) * 0.5

    @pl.loop(0, H // 2 // rows2)
    def _(step):
        r0 = step * rows2
        kept = keep(r0, rows2, HB // 2 + 2 * rows2, band * (HB // 2) - rows2)
        for img in range(2):
            lhs = jnp.concatenate(
                [
                    p1[img, pl.ds(r0 + dr, rows2), k * ph3 : (k + 1) * ph3].reshape(
                        rows2 * ph3 * L, LANES
                    )
                    for dr in range(3)
                    for k in range(2)
                ],
                axis=1,
            )
            h = dot(lhs, w2[...]) + bias
            act = gelu(h)
            for u in range(2):
                lanes = slice(u * C2, (u + 1) * C2)
                a2[img, kept, u] = act[:, lanes].astype(BF16).reshape(rows2, ph3, L, C2)
                if img:
                    z2[kept, u] = h[:, lanes].reshape(rows2, ph3, L, C2)
            s = (act[:, 0:C2] + act[:, C2 : 2 * C2]).reshape(rows2 // 2, 2, ph3, L, C2)
            pooled_into(p2, img, r0 // 2, (s[:, 0] + s[:, 1]) * 0.125)

    copies[0].wait()
    rows3 = ROWS3
    bias3 = b3_ref[...] * 0.5

    @pl.loop(0, H // 4 // rows3)
    def _(step):
        r0 = step * rows3
        kept = keep(r0, rows3, HB // 4 + 2 * rows3, band * (HB // 4) - rows3)
        for img in range(2):
            lhs = three(
                lambda dr, dc: p2[img, pl.ds(r0 + dr, rows3), dc : dc + ph3].reshape(
                    rows3 * ph3 * L, C2
                )
            )
            h = dot(lhs, w3[...]) + bias3
            act = gelu(h)
            a3[img, kept] = act.astype(BF16).reshape(rows3, ph3, L, C3)
            if img:
                z3[kept] = h.reshape(rows3, ph3, L, C3)
            pair = act.reshape(rows3 // 2, 2, ph4, 2, L, C3)
            pooled = (pair[:, 0, :, 0] + pair[:, 0, :, 1]) + (pair[:, 1, :, 0] + pair[:, 1, :, 1])
            pooled_into(p3, img, r0 // 2, pooled * 0.125)

    copies[1].wait()
    rows4 = ROWS4
    bias4 = b4_ref[...] * 0.5

    @pl.loop(0, H // 8 // rows4)
    def _(step):
        r0 = step * rows4
        for img in range(2):
            lhs = three(
                lambda dr, dc: p3[img, pl.ds(r0 + dr, rows4), dc : dc + ph4].reshape(
                    rows4 * ph4 * L, C3
                )
            )
            h = dot(lhs, w4[...]) + bias4
            act = gelu(h)
            at = pl.ds(r0 + 2, rows4)
            a4[img, at] = act.astype(BF16).reshape(rows4, ph4, L, C4)
            if img:
                z4[at] = h.reshape(rows4, ph4, L, C4)
            pair = act.reshape(rows4 // 2, 2, ph4, L, C4)
            pooled = (pair[:, 0, 0] + pair[:, 0, 1]) + (pair[:, 1, 0] + pair[:, 1, 1])
            pooled_into(p4, img, r0 // 2, (pooled * 0.125)[:, None])

    copies[2].wait()
    h5 = H // 16
    lhs = jnp.concatenate(
        [
            three(lambda dr, dc: p4[img, dr : dr + h5, dc].reshape(h5 * L, C4))
            for img in range(2)
        ],
        axis=0,
    )
    h = dot(lhs, w5[...]) + b5_ref[...] * 0.5
    act = gelu(h).astype(BF16)
    for img in range(2):
        a5[img, 2 : 2 + h5, 0] = act[img * h5 * L : (img + 1) * h5 * L].reshape(h5, L, C5)
    z5[2 : 2 + h5, 0] = h[h5 * L :].reshape(h5, L, C5)

    loss_ref[...] = jnp.zeros(loss_ref.shape, F32)
    places = (rows, rows2, rows3, 2 + band * (HB // 8), 2 + band * (HB // 16))
    chunks = (4, 4, 4, 2, 1)
    for s, (acts, l_ref) in enumerate(
        ((a1, l1_ref), (a2, l2_ref), (a3, l3_ref), (a4, l4_ref), (a5, l5_ref))
    ):
        chans = acts.shape[-1]
        ones2 = ones_for(s + 1, chans)
        own, chunk = (HB >> s, chunks[s])
        m = chunk * math.prod(acts.shape[2:-1])
        lin = l_ref[...]
        if s == 0:
            lin = jnp.concatenate([lin, lin], axis=1)

        def piece(k, s=s, acts=acts, ones2=ones2, chunk=chunk, m=m, chans=chans, lin=lin):
            at = pl.ds(places[s] + k * chunk, chunk)
            r = acts[0, at].reshape(m, chans).astype(F32)
            f = acts[1, at].reshape(m, chans).astype(F32)
            inv_r, inv_f = inverse_norms(r, f, ones2, chans)
            d = r * inv_r - f * inv_f
            part = jnp.sum(d * d, axis=0, keepdims=True) * lin
            acc = part[:, 0:LANES]
            for j in range(1, chans // LANES):
                acc = acc + part[:, j * LANES : (j + 1) * LANES]
            loss_ref[s : s + 1, :] += acc

        if own == chunk:
            piece(0)
        else:
            pl.loop(0, own // chunk)(piece)


def taps(seg, acts, pres, grads, l_ref, band, HB, H, up, local, halo, chunk):
    chans = acts.shape[-1]
    inner = acts.shape[2:-1]
    m = chunk * math.prod(inner)
    L = inner[-1]
    own = HB >> (seg - 1)
    total_rows = H >> (seg - 1)
    start = band * own - halo
    scale = -2.0 * 4.0 ** (seg - 1)
    ones2 = ones_for(seg, chans)
    ones1 = ones2[0:LANES, 0:LANES] if seg == 1 else jnp.ones((chans, LANES), BF16)
    reps = chans // LANES
    lin = l_ref[...]
    if seg == 1:
        lin = jnp.concatenate([lin, lin], axis=1)

    def piece(k):
        i0 = k * chunk
        at = pl.ds(local + i0, chunk)
        r = acts[0, at].reshape(m, chans).astype(F32)
        f = acts[1, at].reshape(m, chans).astype(F32)
        inv_r, inv_f = inverse_norms(r, f, ones2, chans)
        nf = f * inv_f
        ld = lin * (r * inv_r - nf)
        q = dot((nf * ld).astype(BF16), ones1)
        if reps > 1:
            q = jnp.concatenate([q] * reps, axis=1)
        tap = (ld - nf * q) * (inv_f * scale)
        if up is not None:
            tap = tap + up(i0, chunk).reshape(m, chans)
        g = gelu_back(pres[at].reshape(m, chans)) * tap
        g = g.reshape((chunk,) + inner + (chans,))
        place = iota(g.shape, 0) + (start + i0)
        g = jnp.where((place >= 0) & (place < total_rows), g, 0.0)
        to = pl.ds(i0, chunk)
        if seg == 2:
            n = inner[1]
            for u in range(2):
                grads[to, u, 1 : n + 1] = g[:, u].astype(BF16)
            grads[to, 1, 0] = shifted(g[:, 1, n - 1], 1).astype(BF16)
            grads[to, 0, n + 1] = shifted(g[:, 0, 0], -1).astype(BF16)
        else:
            n = inner[0]
            grads[to, 1 : n + 1] = g.astype(BF16)
            grads[to, 0] = shifted(g[:, n - 1], 1).astype(BF16)
            grads[to, n + 1] = shifted(g[:, 0], -1).astype(BF16)

    count = own + 2 * halo
    if count == chunk:
        piece(0)
    else:
        pl.loop(0, count // chunk)(piece)


def back5_body(dims, a5, z5, w5, l5, i5, g5):
    H, L, HB, C1, C2, C3, C4, C5 = dims
    band = lax.axis_index("rows")
    own = HB // 16
    taps(5, a5, z5, g5, l5, band, HB, H, None, band * own, 2, own + 4)
    n = own + 2
    lhs = three(lambda dr, dc: g5[dr : dr + n, dc].reshape(n * L, C5))
    rhs = jnp.concatenate([w5[t * C4 : (t + 1) * C4, :] for t in range(8, -1, -1)], axis=1)
    i5[...] = (dot_t(lhs, rhs) * 0.25).reshape(n, 1, L, C4)


def spread_up(ref, axes):
    def load(i0, chunk):
        v = ref[pl.ds(i0 // 2, chunk // 2)]
        n, ph, length, chans = v.shape
        if axes:
            v = jnp.broadcast_to(v[:, None, None], (n, 2, 2, ph, length, chans))
            return v
        return jnp.broadcast_to(v[:, None, :, None], (n, 2, ph, 2, length, chans))

    return load


def back4_body(dims, a4, z4, w4, l4, i5, i4, g4):
    H, L, HB, C1, C2, C3, C4, C5 = dims
    band = lax.axis_index("rows")
    own, ph = (HB // 8, PH // 8)
    taps(4, a4, z4, g4, l4, band, HB, H, spread_up(i5, 0), band * own, 2, 2)
    n = own + 2
    lhs = three(lambda dr, dc: g4[dr : dr + n, dc : dc + ph].reshape(n * ph * L, C4))
    rhs = jnp.concatenate([w4[t * C3 : (t + 1) * C3, :] for t in range(8, -1, -1)], axis=1)
    i4[...] = (dot_t(lhs, rhs) * 0.25).reshape(n, ph, L, C3)


def back3_body(dims, a3, z3, w3, l3, i4, i3, g3):
    H, L, HB, C1, C2, C3, C4, C5 = dims
    band = lax.axis_index("rows")
    own, ph = (HB // 4, PH // 4)
    taps(3, a3, z3, g3, l3, band, HB, H, spread_up(i4, 0), ROWS3 - 2, 2, 4)
    n = own + 2
    lhs = three(lambda dr, dc: g3[dr : dr + n, dc : dc + ph].reshape(n * ph * L, C3))
    rhs = jnp.concatenate([w3[t * C2 : (t + 1) * C2, :] for t in range(8, -1, -1)], axis=1)
    i3[...] = (dot_t(lhs, rhs) * 0.25).reshape(n, ph, L, C2)


def back2_body(dims, a2, z2, w2t, l2, i3, i2, g2):
    H, L, HB, C1, C2, C3, C4, C5 = dims
    band = lax.axis_index("rows")
    own, ph = (HB // 2, PH // 4)
    taps(2, a2, z2, g2, l2, band, HB, H, spread_up(i3, 1), ROWS2 - 2, 2, 4)
    step = (own + 2) // 2
    for r0 in (0, step):
        lhs = jnp.concatenate(
            [
                g2[r0 + dr : r0 + dr + step, 1 - j % 2, (j + 1) // 2 : (j + 1) // 2 + ph].reshape(
                    step * ph * L, C2
                )
                for dr in range(3)
                for j in range(4)
            ],
            axis=1,
        )
        out = (dot_t(lhs, w2t[...]) * 0.25).reshape(step, ph, L, 2 * LANES)
        for u in range(2):
            i2[r0 : r0 + step, u] = out[..., u * LANES : (u + 1) * LANES]


def back1_body(dims, a1, z1, r1, l1, i2, grad_ref, g1):
    H, L, HB, C1, C2, C3, C4, C5 = dims
    band = lax.axis_index("rows")
    ph = PH // 4

    def up(i0, chunk):
        v = i2[pl.ds(i0 // 2, chunk // 2 + 1)]
        v = jnp.stack([v[:, q % 2, q // 2] for q in range(2 * ph)], axis=1)
        return jnp.stack([v[(j + 1) // 2] for j in range(chunk)])

    taps(1, a1, z1, g1, l1, band, HB, H, up, ROWS1 - 1, 1, 6)
    lhs = jnp.concatenate(
        [g1[dr : dr + HB, j].reshape(HB * L, LANES) for dr in range(3) for j in range(PH // 2 + 2)],
        axis=1,
    )
    gin = dot_t(lhs, r1[...])
    high = gin.astype(BF16)
    split = jnp.concatenate([high.astype(F32), gin - high.astype(F32)], axis=1).astype(BF16)
    width = PH * L
    sel_row = iota((LANES, width), 0) % HALF
    sel_col = iota((LANES, width), 1) % PH
    shape = (HB * L, width)
    inside = iota(shape, 1) // PH == iota(shape, 0) % L
    for ch in range(3):
        pick = jnp.where(sel_row == sel_col * 3 + ch, 1.0, 0.0).astype(BF16)
        wide = jnp.where(inside, dot(split, pick), 0.0)
        grad_ref[ch] = jnp.sum(wide.reshape(HB, L, width), axis=1)


ROWS1, ROWS2, ROWS3, ROWS4 = (8, 4, 4, 4)


def frame_work(x, c1, c2, b1, convs, biases, linears, HB):
    H, L, _ = x.shape
    C1, C2, C3, C4, C5 = [c.shape[-1] for c in convs]
    dims = (H, L, HB, C1, C2, C3, C4, C5)
    ph2, ph3, ph4 = (PH // 2, PH // 4, PH // 8)
    V = pltpu.VMEM
    far = [c.reshape(-1, c.shape[-1]) for c in convs[2:]]
    far += [v.reshape(1, -1) for v in (*biases[1:], *linears)]
    w1, r1, w2, w2t = call(
        weights_body,
        (
            V((4 * HALF, PH * HALF), BF16),
            V((HALF, 3 * (ph2 + 2) * LANES), BF16),
            V((12 * C1, 2 * C2), BF16),
            V((4 * C1, 12 * C2), BF16),
        ),
        (c1, c2, b1),
        "weights",
        (V((3, HALF, LANES), F32), V((8, LANES), F32)),
        limit=8,
    )
    acts = (
        (HB + 3 * ROWS1, ph2, L, LANES),
        (HB // 2 + 3 * ROWS2, 2, ph3, L, C2),
        (HB // 4 + 3 * ROWS3, ph3, L, C3),
        (H // 8 + 4, ph4, L, C4),
        (H // 16 + 4, 1, L, C5),
    )
    outs = (V((8, LANES), F32),)
    outs += tuple(V((2,) + s, BF16) for s in acts) + tuple(V(s, F32) for s in acts)
    outs += tuple(V(v.shape, v.dtype) for v in far)
    loss, a1, a2, a3, a4, a5, z1, z2, z3, z4, z5, w3, w4, w5, *vecs = call(
        functools.partial(forward_body, dims),
        outs,
        (x, w1, w2),
        "forward",
        (
            V((2, H, L, 2 * LANES), BF16),
            V((2, H // 2 + 2, ph2, L, LANES), BF16),
            V((2, H // 4 + 2, ph3 + 2, L, C2), BF16),
            V((2, H // 8 + 2, ph4 + 2, L, C3), BF16),
            V((2, H // 16 + 2, 3, L, C4), BF16),
            pltpu.SemaphoreType.DMA((12,)),
        ),
        limit=24,
        far=far,
    )
    l = vecs[4:]
    n1, n2, n3, n4, n5 = (HB + 2, HB // 2 + 4, HB // 4 + 4, HB // 8 + 4, HB // 16 + 4)

    def step(body, name, ins, out, scratch, flops):
        return call(functools.partial(body, dims), out, ins, name, (V(scratch, BF16),), 12, flops)

    def back5(_):
        return step(
            back5_body, "back5", (a5, z5, w5, l[4]), V((n5 - 2, 1, L, C4), F32), (n5, 3, L, C5), FL
        )

    def back4(i5):
        return step(
            back4_body, "back4", (a4, z4, w4, l[3], i5), V((n4 - 2, ph4, L, C3), F32),
            (n4, ph4 + 2, L, C4), FL,
        )

    def back3(i4):
        return step(
            back3_body, "back3", (a3, z3, w3, l[2], i4), V((n3 - 2, ph3, L, C2), F32),
            (n3, ph3 + 2, L, C3), FL,
        )

    def back2(i3):
        return step(
            back2_body, "back2", (a2, z2, w2t, l[1], i3), V((n2 - 2, 2, ph3, L, LANES), F32),
            (n2, 2, ph3 + 2, L, C2), FL,
        )

    def back1(i2):
        return step(
            back1_body, "back1", (a1, z1, r1, l[0], i2),
            jax.ShapeDtypeStruct((3, HB, L * PH), F32), (n1, ph2 + 2, L, LANES), FL,
        )

    return loss, (back5, back4, back3, back2, back1)


FL = 10**9


def on_device(real_frames, fake_frames, *params):
    convs, biases, linears = (params[0:5], params[5:10], params[10:15])
    frames, _, band_rows, width = real_frames.shape
    bands = lax.axis_size("rows")
    frame_total = frames * lax.axis_size("dp")
    work = []
    for n in range(frames):
        c1, c2, b1 = (convs[0], convs[1], biases[0].reshape(1, -1))
        c2 = c2.reshape(9, *c2.shape[2:])
        x, c1, c2, b1 = prep(real_frames[n], fake_frames[n], c1, c2, b1)
        x = lax.all_gather(x, "rows", axis=0, tiled=True)
        work.append(frame_work(x, c1, c2, b1, convs, biases, linears, band_rows))
    total = functools.reduce(jnp.add, [loss for loss, _ in work])
    hops = []
    for axis in ("rows", "dp"):
        hop = 1
        while hop < lax.axis_size(axis):
            hops.append((axis, hop))
            hop *= 2
    states = [None] * frames
    for stage in range(max(5, len(hops))):
        if stage < len(hops):
            axis, hop = hops[stage]
            pairs = [(i, i ^ hop) for i in range(lax.axis_size(axis))]
            other = lax.ppermute(total, axis, pairs)
        if stage < 5:
            states = [steps[stage](s) for s, (_, steps) in zip(states, work)]
        if stage < len(hops):
            total, other, states = lax.optimization_barrier((total, other, states))
            total = total + other
    counts = [frame_total * (band_rows * bands >> s) * (width >> s) for s in range(5)]
    losses = jnp.sum(total, axis=1)[0:5] * jnp.array([1.0 / c for c in counts], F32)
    return (losses, jnp.stack(states))


def solution(mesh):
    frame = P("dp", None, "rows", None)
    return jax.shard_map(
        on_device,
        mesh=mesh,
        in_specs=(frame, frame) + (P(),) * 15,
        out_specs=(P(), frame),
        check_vma=False,
    )
```

```python
import functools
import math

import jax
import jax.numpy as jnp
from jax import lax
from jax.experimental import pallas as pl
from jax.experimental.pallas import tpu as pltpu
from jax.sharding import PartitionSpec as P

EPS = 1e-06
F32 = jnp.float32
BF16 = jnp.bfloat16
K0 = math.sqrt(2.0 / math.pi)
K1 = K0 * 0.044715
PH = 16
LANES = 128
HALF = 64
ONE = (PH + 2) * 3
MIB = 1 << 20
VM = pl.BlockSpec(memory_space=pltpu.VMEM)
HBM = pl.BlockSpec(memory_space=pltpu.HBM)


def gelu(h):
    t = jnp.tanh(h * (2.0 * K0 + (8.0 * K1) * (h * h)))
    return h + h * t


def gelu_back(h):
    sq = h * h
    t = jnp.tanh(h * (2.0 * K0 + (8.0 * K1) * sq))
    return (0.5 + 0.5 * t) + (h * (1.0 - t * t)) * (K0 + (12.0 * K1) * sq)


def dot(a, b):
    return lax.dot_general(a, b, (((1,), (0,)), ((), ())), preferred_element_type=F32)


def dot_t(a, b):
    return lax.dot_general(a, b, (((1,), (1,)), ((), ())), preferred_element_type=F32)


def iota(shape, dim):
    return lax.broadcasted_iota(jnp.int32, shape, dim)


def low_half(shape):
    return iota(shape, len(shape) - 1) % LANES < HALF


def shifted(value, step):
    n, length, chans = value.shape
    flat = value.reshape(n * length, chans)
    place = iota(flat.shape, 0) % length
    if step > 0:
        out = jnp.where(place == 0, 0.0, pltpu.roll(flat, 1, 0))
    else:
        out = jnp.where(place == length - 1, 0.0, pltpu.roll(flat, n * length - 1, 0))
    return out.reshape(n, length, chans)


def call(body, outs, ins, name, scratch=(), limit=16, flops=0, far=()):
    far = [pltpu.with_memory_space_constraint(v, pltpu.HBM) for v in far]
    return pl.pallas_call(
        body,
        out_shape=outs,
        in_specs=[HBM] * len(far) + [VM] * len(ins),
        out_specs=jax.tree.map(lambda _: VM, outs),
        scratch_shapes=scratch,
        name=name,
        cost_estimate=pl.CostEstimate(flops=flops, transcendentals=0, bytes_accessed=0),
        compiler_params=pltpu.CompilerParams(vmem_limit_bytes=limit * MIB),
    )(*far, *ins)


def prep_body(
    real_hbm, fake_hbm, c1_hbm, c2_hbm, b1_hbm,
    out_ref, c1, c2, b1, real_ref, fake_ref, sems,
):
    pairs = ((real_hbm, real_ref), (fake_hbm, fake_ref), (c1_hbm, c1), (c2_hbm, c2), (b1_hbm, b1))
    copies = [pltpu.make_async_copy(a, b, sems.at[i]) for i, (a, b) in enumerate(pairs)]
    for copy in copies:
        copy.start()
    _, rows, width = real_ref.shape
    length = width // PH
    shape = (rows * length, width)
    col = iota(shape, 1)
    place = iota(shape, 0) % length
    inside = col // PH == place
    edges = (col == place * PH - 1) | (col == place * PH + PH)
    eshape = (width, LANES)
    ecol = iota(eshape, 0) % PH
    lane = iota(eshape, 1)
    total = jnp.zeros((rows * length, LANES), F32)
    for copy in copies:
        copy.wait()
    for img, ref in enumerate((real_ref, fake_ref)):
        for ch in range(3):
            x = ref[ch].astype(F32)
            wide = jnp.broadcast_to(x[:, None, :], (rows, length, width)).reshape(shape)
            base = img * HALF + ch
            a = jnp.concatenate(
                [jnp.where(inside, wide, 0.0), jnp.where(edges, wide, 0.0)], axis=1
            ).astype(BF16)
            e_in = lane == base + (ecol + 1) * 3
            e_edge = ((ecol == PH - 1) & (lane == base)) | (
                (ecol == 0) & (lane == base + (PH + 1) * 3)
            )
            e = jnp.concatenate(
                [jnp.where(e_in, 1.0, 0.0), jnp.where(e_edge, 1.0, 0.0)], axis=0
            ).astype(BF16)
            total = total + dot(a, e)
    lane = iota(total.shape, 1) % HALF
    total = jnp.where((lane >= ONE) & (lane < ONE + 3), 1.0, total)
    out_ref[...] = total.astype(BF16).reshape(rows, length, LANES)


def prep(real, fake, c1, c2, b1):
    _, rows, width = real.shape
    V = pltpu.VMEM
    return call(
        prep_body,
        (V((rows, width // PH, LANES), BF16), V(c1.shape, BF16), V(c2.shape, BF16), V(b1.shape, F32)),
        (),
        "prep",
        (V(real.shape, BF16), V(fake.shape, BF16), pltpu.SemaphoreType.DMA((5,))),
        limit=8,
        far=(real, fake, c1, c2, b1),
    )


def weights_body(c1_ref, c2_ref, b1_ref, w1, r1, w2, w2t, base, bias):
    C1, C2 = c2_ref.shape[1:]
    base[...] = jnp.zeros(base.shape, F32)
    for dr in range(3):
        for dc in range(3):
            blk = c1_ref[dr, dc].astype(F32)
            base[dr, dc * 3 : dc * 3 + 3, 0:HALF] = blk
            base[dr, dc * 3 : dc * 3 + 3, HALF:LANES] = blk
    bias[0:1, 0:HALF] = b1_ref[...]
    bias[0:1, HALF:LANES] = b1_ref[...]
    left = bias[0:1, :]
    shape = (HALF, LANES)
    row = iota(shape, 0)
    lo = low_half(shape)
    extra = jnp.zeros(shape, F32)
    for k in range(3):
        part = left.astype(BF16).astype(F32)
        extra = jnp.where(row == ONE + k, jnp.broadcast_to(part, shape), extra)
        left = left - part
    for dr in range(3):
        b = base[dr]
        for i in range(PH // 2):
            first = pltpu.roll(b, (6 * i) % HALF, 0) if i else b
            blk = jnp.where(lo, first, pltpu.roll(b, (6 * i + 3) % HALF, 0))
            if dr == 1:
                blk = blk + extra
            w1[dr * HALF : (dr + 1) * HALF, i * LANES : (i + 1) * LANES] = (0.5 * blk).astype(BF16)
        b = base[2 - dr]
        for j in range(PH // 2 + 2):
            s0, s1 = ((6 * j - 9) % HALF, (6 * j - 6) % HALF)
            blk = jnp.where(
                lo, pltpu.roll(b, s0, 0) if s0 else b, pltpu.roll(b, s1, 0) if s1 else b
            )
            r1[dr * HALF : (dr + 1) * HALF, j * LANES : (j + 1) * LANES] = blk.astype(BF16)
    w1[3 * HALF : 4 * HALF, :] = jnp.zeros((HALF, w1.shape[1]), BF16)
    r1[3 * HALF : 4 * HALF, :] = jnp.zeros((HALF, r1.shape[1]), BF16)
    w2[...] = jnp.zeros(w2.shape, BF16)
    w2t[...] = jnp.zeros(w2t.shape, BF16)
    slot = (2, 0, 1, 3)
    for dr in range(3):
        for dc in range(3):
            blk = c2_ref[dr * 3 + dc]
            back = c2_ref[(2 - dr) * 3 + 2 - dc]
            for u in range(2):
                k = (dr * 4 + slot[dc + u]) * C1
                w2[k : k + C1, u * C2 : (u + 1) * C2] = (blk.astype(F32) * 0.125).astype(BF16)
                k = (dr * 4 + dc + u) * C2
                for d in range(2):
                    n = (u * 2 + d) * C1
                    w2t[n : n + C1, k : k + C2] = back


def three(load):
    return jnp.concatenate([load(dr, dc) for dr in range(3) for dc in range(3)], axis=1)


def pooled_into(ref, img, row, value):
    rows, phases = value.shape[0:2]
    at = pl.ds(row + 1, rows)
    ref[img, at, 1 : phases + 1] = value.astype(BF16)
    ref[img, at, 0] = shifted(value[:, phases - 1], 1).astype(BF16)
    ref[img, at, phases + 1] = shifted(value[:, 0], -1).astype(BF16)


def inverse_norms(r, f, ones2, chans):
    sums = dot(jnp.concatenate([r * r, f * f], axis=1).astype(BF16), ones2)
    reps = chans // LANES

    def spread(v):
        return jnp.concatenate([v] * reps, axis=1) if reps > 1 else v

    inv = lax.rsqrt(sums + EPS)
    return spread(inv[:, 0:LANES]), spread(inv[:, LANES : 2 * LANES])


def ones_for(seg, chans):
    rr = iota((2 * chans, 2 * LANES), 0)
    cc = iota((2 * chans, 2 * LANES), 1)
    if seg == 1:
        return jnp.where(rr // HALF == cc // HALF, 1.0, 0.0).astype(BF16)
    return jnp.where(rr // chans == cc // LANES, 1.0, 0.0).astype(BF16)


def forward_body(
    dims,
    *refs,
):
    H, L, HB, C1, C2, C3, C4, C5 = dims
    far, refs = (refs[0:12], refs[12:])
    blocks, refs = (refs[0 : H // HB], refs[H // HB :])
    w1, w2, loss_ref, t1, t2, t3, t4, t5, z1, z2, z3, z4, z5 = refs[0:13]
    near, refs = (refs[13:25], refs[25:])
    w3, w4, w5, b2_ref, b3_ref, b4_ref, b5_ref, *l_refs = near
    xs, xk, p1, p2, p3, p4, a1, a2, a3, a4, a5, sems = refs
    copies = [pltpu.make_async_copy(a, b, sems.at[i]) for i, (a, b) in enumerate(zip(far, near))]
    for copy in copies[3:] + copies[:3]:
        copy.start()
    ph2, ph3, ph4 = (PH // 2, PH // 4, PH // 8)
    band = lax.axis_index("rows")
    for p in (p1, p2, p3, p4):
        n = p.shape[1]
        for img in range(2):
            p[img, 0] = jnp.zeros(p.shape[2:], BF16)
            p[img, n - 1] = jnp.zeros(p.shape[2:], BF16)

    xs[0] = jnp.zeros((L, LANES), BF16)
    xs[H + 1] = jnp.zeros((L, LANES), BF16)
    for m, block in enumerate(blocks):
        xs[pl.ds((band ^ m) * HB + 1, HB)] = block[...]
    x = xs[...].astype(F32)
    xr = pltpu.roll(x.reshape((H + 2) * L, LANES), HALF, 1).reshape(H + 2, L, LANES)
    lo3 = low_half((H, L, LANES))
    xk[0, :, :, 0:LANES] = jnp.where(lo3, x[0:H], xr[1 : H + 1]).astype(BF16)
    xk[0, :, :, LANES : 2 * LANES] = x[2 : H + 2].astype(BF16)
    xk[1, :, :, 0:LANES] = jnp.where(lo3, xr[0:H], x[1 : H + 1]).astype(BF16)
    xk[1, :, :, LANES : 2 * LANES] = xr[2 : H + 2].astype(BF16)

    def keep(r0, rows, size, first):
        place = r0 - first
        return pl.ds(jnp.where((place >= 0) & (place < size), place, size), rows)

    rows = ROWS1

    @pl.loop(0, H // rows, unroll=2)
    def _(step):
        r0 = step * rows
        kept = keep(r0, rows, HB + 2 * rows, band * HB - rows)
        at = pl.ds(r0 // 2 + 1, rows // 2)
        for img in range(2):
            lhs = xk[img, pl.ds(r0, rows)].reshape(rows * L, 2 * LANES)
            for n in range(PH // 4):
                h = dot(lhs, w1[:, n * 256 : (n + 1) * 256])
                act = gelu(h)
                for i in range(2):
                    lanes = slice(i * LANES, (i + 1) * LANES)
                    part = act[:, lanes].reshape(rows, L, LANES)
                    a1[img, kept, n * 2 + i] = part.astype(BF16)
                    if img:
                        z1[kept, n * 2 + i] = h[:, lanes].reshape(rows, L, LANES)
                    pair = part.reshape(rows // 2, 2, L, LANES)
                    s = (pair[:, 0] + pair[:, 1]).reshape(rows // 2 * L, LANES)
                    s = (s + pltpu.roll(s, HALF, 1)).reshape(rows // 2, L, LANES)
                    half = slice(i * HALF, (i + 1) * HALF)
                    p1[img, at, n, :, half] = s.astype(BF16)[..., half]
                    q = n * 2 + i
                    other = slice((1 - i) * HALF, (2 - i) * HALF)
                    if q == ph2 - 1:
                        s = shifted(s, 1)
                    if q == 0:
                        s = shifted(s, -1)
                    slot = ph3 + (n + 1 if i else n - 1) % ph3
                    p1[img, at, slot, :, other] = s.astype(BF16)[..., other]

    for copy in copies[3:]:
        copy.wait()

    rows2, rows3, rows4 = (ROWS2, ROWS3, ROWS4)
    loss_ref[...] = jnp.zeros(loss_ref.shape, F32)
    places = (rows - 1, rows2 - 2, rows3 - 2, band * (HB // 8), band * (HB // 16))

    def tap(seg):
        s = seg - 1
        acts = (a1, a2, a3, a4, a5)[s]
        taps(seg, acts, (t1, t2, t3, t4, t5)[s], l_refs[s], loss_ref, HB >> s, places[s])

    for copy in copies[:3]:
        copy.wait()
    tap(1)
    bias = jnp.concatenate([b2_ref[...]] * 2, axis=1) * 0.5

    for step in range(H // 2 // rows2):
        r0 = step * rows2
        kept = keep(r0, rows2, HB // 2 + 2 * rows2, band * (HB // 2) - rows2)
        for img in range(2):
            lhs = jnp.concatenate(
                [
                    p1[img, pl.ds(r0 + dr, rows2), k * ph3 : (k + 1) * ph3].reshape(
                        rows2 * ph3 * L, LANES
                    )
                    for dr in range(3)
                    for k in range(2)
                ],
                axis=1,
            )
            h = dot(lhs, w2[...]) + bias
            act = gelu(h)
            for u in range(2):
                lanes = slice(u * C2, (u + 1) * C2)
                a2[img, kept, u] = act[:, lanes].astype(BF16).reshape(rows2, ph3, L, C2)
                if img:
                    z2[kept, u] = h[:, lanes].reshape(rows2, ph3, L, C2)
            s = (act[:, 0:C2] + act[:, C2 : 2 * C2]).reshape(rows2 // 2, 2, ph3, L, C2)
            pooled_into(p2, img, r0 // 2, (s[:, 0] + s[:, 1]) * 0.125)

    tap(2)
    bias3 = b3_ref[...] * 0.5

    for step in range(H // 4 // rows3):
        r0 = step * rows3
        kept = keep(r0, rows3, HB // 4 + 2 * rows3, band * (HB // 4) - rows3)
        for img in range(2):
            lhs = three(
                lambda dr, dc: p2[img, pl.ds(r0 + dr, rows3), dc : dc + ph3].reshape(
                    rows3 * ph3 * L, C2
                )
            )
            h = dot(lhs, w3[...]) + bias3
            act = gelu(h)
            a3[img, kept] = act.astype(BF16).reshape(rows3, ph3, L, C3)
            if img:
                z3[kept] = h.reshape(rows3, ph3, L, C3)
            pair = act.reshape(rows3 // 2, 2, ph4, 2, L, C3)
            pooled = (pair[:, 0, :, 0] + pair[:, 0, :, 1]) + (pair[:, 1, :, 0] + pair[:, 1, :, 1])
            pooled_into(p3, img, r0 // 2, pooled * 0.125)

    tap(3)
    bias4 = b4_ref[...] * 0.5

    for step in range(H // 8 // rows4):
        r0 = step * rows4
        lhs = jnp.concatenate(
            [
                three(
                    lambda dr, dc, img=img: p3[
                        img, pl.ds(r0 + dr, rows4), dc : dc + ph4
                    ].reshape(rows4 * ph4 * L, C3)
                )
                for img in range(2)
            ],
            axis=0,
        )
        m = rows4 * ph4 * L
        at = pl.ds(r0 + 2, rows4)
        to = pl.ds(r0 // 2 + 1, rows4 // 2)
        for n in range(0, C4, 256):
            lanes = slice(n, n + 256)
            both = dot(lhs, w4[:, lanes]) + bias4[:, lanes]
            for img in range(2):
                h = both[img * m : (img + 1) * m]
                act = gelu(h)
                a4[img, at, :, :, lanes] = act.astype(BF16).reshape(rows4, ph4, L, 256)
                if img:
                    z4[at, :, :, lanes] = h.reshape(rows4, ph4, L, 256)
                pair = act.reshape(rows4 // 2, 2, ph4, L, 256)
                pooled = (pair[:, 0, 0] + pair[:, 0, 1]) + (pair[:, 1, 0] + pair[:, 1, 1])
                pooled = pooled * 0.125
                p4[img, to, 1, :, lanes] = pooled.astype(BF16)
                p4[img, to, 0, :, lanes] = shifted(pooled, 1).astype(BF16)
                p4[img, to, 2, :, lanes] = shifted(pooled, -1).astype(BF16)

    tap(4)
    h5 = H // 16
    lhs = jnp.concatenate(
        [
            three(lambda dr, dc: p4[img, dr : dr + h5, dc].reshape(h5 * L, C4))
            for img in range(2)
        ],
        axis=0,
    )
    h = dot(lhs, w5[...]) + b5_ref[...] * 0.5
    act = gelu(h).astype(BF16)
    for img in range(2):
        a5[img, 2 : 2 + h5, 0] = act[img * h5 * L : (img + 1) * h5 * L].reshape(h5, L, C5)
    z5[2 : 2 + h5, 0] = h[h5 * L :].reshape(h5, L, C5)
    tap(5)


def taps(seg, acts, grads, l_ref, loss_ref, own, local):
    chans = acts.shape[-1]
    inner = acts.shape[2:-1]
    halo = 1 if seg == 1 else 2
    count = own + 2 * halo
    chunk = TAP_ROWS[seg - 1] or count
    m = chunk * math.prod(inner)
    scale = -2.0 * 4.0 ** (seg - 1)
    ones2 = ones_for(seg, chans)
    ones1 = ones2[0:LANES, 0:LANES] if seg == 1 else jnp.ones((chans, LANES), BF16)
    reps = chans // LANES
    lin = l_ref[...]
    if seg == 1:
        lin = jnp.concatenate([lin, lin], axis=1)

    def piece(k):
        i0 = k * chunk
        at = pl.ds(local + i0, chunk)
        r = acts[0, at].reshape(m, chans).astype(F32)
        f = acts[1, at].reshape(m, chans).astype(F32)
        inv_r, inv_f = inverse_norms(r, f, ones2, chans)
        nf = f * inv_f
        d = r * inv_r - nf
        ld = lin * d
        q = dot((nf * ld).astype(BF16), ones1)
        if reps > 1:
            q = jnp.concatenate([q] * reps, axis=1)
        tap = (ld - nf * q) * (inv_f * scale)
        grads[pl.ds(i0, chunk)] = tap.reshape((chunk,) + inner + (chans,))
        mapped = (ld * d).reshape((chunk,) + inner + (chans,))
        place = iota(mapped.shape, 0) + i0
        mapped = jnp.where((place >= halo) & (place < halo + own), mapped, 0.0)
        part = jnp.sum(mapped.reshape(m, chans), axis=0, keepdims=True)
        acc = part[:, 0:LANES]
        for j in range(1, reps):
            acc = acc + part[:, j * LANES : (j + 1) * LANES]
        loss_ref[seg - 1 : seg, :] += acc

    for k in range(count // chunk):
        piece(k)


def pre_grads(seg, tap_ref, pres, grads, band, HB, H, up, local, halo, chunk):
    chans = pres.shape[-1]
    inner = pres.shape[1:-1]
    own = HB >> (seg - 1)
    total_rows = H >> (seg - 1)
    start = band * own - halo
    shape = (chunk,) + inner + (chans,)

    def piece(k):
        i0 = k * chunk
        g = tap_ref[pl.ds(i0, chunk)]
        if up is not None:
            g = g + up(i0, chunk).reshape(shape)
        g = gelu_back(pres[pl.ds(local + i0, chunk)]) * g
        place = iota(shape, 0) + (start + i0)
        g = jnp.where((place >= 0) & (place < total_rows), g, 0.0)
        to = pl.ds(i0, chunk)
        if seg == 2:
            n = inner[1]
            for u in range(2):
                grads[to, u, 1 : n + 1] = g[:, u].astype(BF16)
            grads[to, 1, 0] = shifted(g[:, 1, n - 1], 1).astype(BF16)
            grads[to, 0, n + 1] = shifted(g[:, 0, 0], -1).astype(BF16)
        else:
            n = inner[0]
            grads[to, 1 : n + 1] = g.astype(BF16)
            grads[to, 0] = shifted(g[:, n - 1], 1).astype(BF16)
            grads[to, n + 1] = shifted(g[:, 0], -1).astype(BF16)

    count = own + 2 * halo
    if count == chunk:
        piece(0)
    else:
        pl.loop(0, count // chunk)(piece)


def back5_body(dims, t5, z5, w5, i5, g5):
    H, L, HB, C1, C2, C3, C4, C5 = dims
    band = lax.axis_index("rows")
    own = HB // 16
    pre_grads(5, t5, z5, g5, band, HB, H, None, band * own, 2, own + 4)
    n = own + 2
    lhs = three(lambda dr, dc: g5[dr : dr + n, dc].reshape(n * L, C5))
    rhs = jnp.concatenate([w5[t * C4 : (t + 1) * C4, :] for t in range(8, -1, -1)], axis=1)
    i5[...] = (dot_t(lhs, rhs) * 0.25).reshape(n, 1, L, C4)


def spread_up(ref, axes):
    def load(i0, chunk):
        v = ref[pl.ds(i0 // 2, chunk // 2)]
        n, ph, length, chans = v.shape
        if axes:
            v = jnp.broadcast_to(v[:, None, None], (n, 2, 2, ph, length, chans))
            return v
        return jnp.broadcast_to(v[:, None, :, None], (n, 2, ph, 2, length, chans))

    return load


def back4_body(dims, t4, z4, w4, i5, i4, g4):
    H, L, HB, C1, C2, C3, C4, C5 = dims
    band = lax.axis_index("rows")
    own, ph = (HB // 8, PH // 8)
    pre_grads(4, t4, z4, g4, band, HB, H, spread_up(i5, 0), band * own, 2, own + 4)
    n = own + 2
    lhs = three(lambda dr, dc: g4[dr : dr + n, dc : dc + ph].reshape(n * ph * L, C4))
    rhs = jnp.concatenate([w4[t * C3 : (t + 1) * C3, :] for t in range(8, -1, -1)], axis=1)
    i4[...] = (dot_t(lhs, rhs) * 0.25).reshape(n, ph, L, C3)


def back3_body(dims, t3, z3, w3, i4, i3, g3):
    H, L, HB, C1, C2, C3, C4, C5 = dims
    band = lax.axis_index("rows")
    own, ph = (HB // 4, PH // 4)
    pre_grads(3, t3, z3, g3, band, HB, H, spread_up(i4, 0), ROWS3 - 2, 2, own + 4)
    n = own + 2
    lhs = three(lambda dr, dc: g3[dr : dr + n, dc : dc + ph].reshape(n * ph * L, C3))
    rhs = jnp.concatenate([w3[t * C2 : (t + 1) * C2, :] for t in range(8, -1, -1)], axis=1)
    i3[...] = (dot_t(lhs, rhs) * 0.25).reshape(n, ph, L, C2)


def back2_body(dims, t2, z2, w2t, i3, i2, g2):
    H, L, HB, C1, C2, C3, C4, C5 = dims
    band = lax.axis_index("rows")
    own, ph = (HB // 2, PH // 4)
    pre_grads(2, t2, z2, g2, band, HB, H, spread_up(i3, 1), ROWS2 - 2, 2, 6)
    step = (own + 2) // 2
    for r0 in (0, step):
        lhs = jnp.concatenate(
            [
                g2[r0 + dr : r0 + dr + step, 1 - j % 2, (j + 1) // 2 : (j + 1) // 2 + ph].reshape(
                    step * ph * L, C2
                )
                for dr in range(3)
                for j in range(4)
            ],
            axis=1,
        )
        out = (dot_t(lhs, w2t[...]) * 0.25).reshape(step, ph, L, 2 * LANES)
        for u in range(2):
            i2[r0 : r0 + step, u] = out[..., u * LANES : (u + 1) * LANES]


def back1_body(dims, t1, z1, r1, i2, grad_ref, g1):
    H, L, HB, C1, C2, C3, C4, C5 = dims
    band = lax.axis_index("rows")
    ph = PH // 4

    def up(i0, chunk):
        v = i2[pl.ds(i0 // 2, chunk // 2 + 1)]
        v = jnp.stack([v[:, q % 2, q // 2] for q in range(2 * ph)], axis=1)
        return jnp.stack([v[(j + 1) // 2] for j in range(chunk)])

    pre_grads(1, t1, z1, g1, band, HB, H, up, ROWS1 - 1, 1, 6)
    lhs = jnp.concatenate(
        [g1[:, j].reshape((HB + 2) * L, LANES) for j in range(PH // 2 + 2)], axis=1
    )
    rows3 = dot_t(lhs, r1[...]).reshape(HB + 2, L, 2 * LANES)
    first = rows3[0:HB, :, 0:LANES].reshape(HB * L, LANES)
    second = rows3[1 : HB + 1, :, 0:LANES].reshape(HB * L, LANES)
    third = rows3[2 : HB + 2, :, LANES : 2 * LANES].reshape(HB * L, LANES)
    gin = (first + pltpu.roll(second, HALF, 1) + third)[:, 0:HALF]
    high = gin.astype(BF16)
    split = jnp.concatenate([high.astype(F32), gin - high.astype(F32)], axis=1).astype(BF16)
    width = PH * L
    sel_row = iota((LANES, width), 0) % HALF
    sel_col = iota((LANES, width), 1) % PH
    shape = (HB * L, width)
    inside = iota(shape, 1) // PH == iota(shape, 0) % L
    for ch in range(3):
        pick = jnp.where(sel_row == sel_col * 3 + ch, 1.0, 0.0).astype(BF16)
        wide = jnp.where(inside, dot(split, pick), 0.0)
        grad_ref[ch] = jnp.sum(wide.reshape(HB, L, width), axis=1)


ROWS1, ROWS2, ROWS3, ROWS4 = (8, 4, 4, 8)
TAP_ROWS = (6, 4, 4, 0, 0)


def frame_work(x, c1, c2, b1, convs, biases, linears, HB):
    H, L, _ = x[0].shape
    H = H * len(x)
    C1, C2, C3, C4, C5 = [c.shape[-1] for c in convs]
    dims = (H, L, HB, C1, C2, C3, C4, C5)
    ph2, ph3, ph4 = (PH // 2, PH // 4, PH // 8)
    V = pltpu.VMEM
    far = [c.reshape(-1, c.shape[-1]) for c in convs[2:]]
    far += [v.reshape(1, -1) for v in (*biases[1:], *linears)]
    w1, r1, w2, w2t = call(
        weights_body,
        (
            V((4 * HALF, PH * HALF), BF16),
            V((4 * HALF, (ph2 + 2) * LANES), BF16),
            V((12 * C1, 2 * C2), BF16),
            V((4 * C1, 12 * C2), BF16),
        ),
        (c1, c2, b1),
        "weights",
        (V((3, HALF, LANES), F32), V((8, LANES), F32)),
        limit=8,
    )
    acts = (
        (HB + 3 * ROWS1, ph2, L, LANES),
        (HB // 2 + 3 * ROWS2, 2, ph3, L, C2),
        (HB // 4 + 3 * ROWS3, ph3, L, C3),
        (H // 8 + 4, ph4, L, C4),
        (H // 16 + 4, 1, L, C5),
    )
    outs = (V((8, LANES), F32),)
    halos = (1, 2, 2, 2, 2)
    outs += tuple(V(((HB >> i) + 2 * halos[i],) + s[1:], F32) for i, s in enumerate(acts))
    outs += tuple(V(s, F32) for s in acts)
    outs += tuple(V(v.shape, v.dtype) for v in far)
    loss, t1, t2, t3, t4, t5, z1, z2, z3, z4, z5, w3, w4, w5, *_ = call(
        functools.partial(forward_body, dims),
        outs,
        (*x, w1, w2),
        "forward",
        (
            V((H + 2, L, LANES), BF16),
            V((2, H, L, 2 * LANES), BF16),
            V((2, H // 2 + 2, ph2, L, LANES), BF16),
            V((2, H // 4 + 2, ph3 + 2, L, C2), BF16),
            V((2, H // 8 + 2, ph4 + 2, L, C3), BF16),
            V((2, H // 16 + 2, 3, L, C4), BF16),
            *[V((2,) + s, BF16) for s in acts],
            pltpu.SemaphoreType.DMA((12,)),
        ),
        limit=32,
        far=far,
    )
    n1, n2, n3, n4, n5 = (HB + 2, HB // 2 + 4, HB // 4 + 4, HB // 8 + 4, HB // 16 + 4)

    def step(body, name, ins, out, scratch, flops):
        return call(functools.partial(body, dims), out, ins, name, (V(scratch, BF16),), 12, flops)

    def back5(_):
        return step(
            back5_body, "back5", (t5, z5, w5), V((n5 - 2, 1, L, C4), F32), (n5, 3, L, C5), FL
        )

    def back4(i5):
        return step(
            back4_body, "back4", (t4, z4, w4, i5), V((n4 - 2, ph4, L, C3), F32),
            (n4, ph4 + 2, L, C4), FL,
        )

    def back3(i4):
        return step(
            back3_body, "back3", (t3, z3, w3, i4), V((n3 - 2, ph3, L, C2), F32),
            (n3, ph3 + 2, L, C3), FL,
        )

    def back2(i3):
        return step(
            back2_body, "back2", (t2, z2, w2t, i3), V((n2 - 2, 2, ph3, L, LANES), F32),
            (n2, 2, ph3 + 2, L, C2), FL,
        )

    def back1(i2):
        return step(
            back1_body, "back1", (t1, z1, r1, i2),
            jax.ShapeDtypeStruct((3, HB, L * PH), F32), (n1, ph2 + 2, L, LANES), FL,
        )

    return loss, (back5, back4, back3, back2, back1)


FL = 10**9


def sum_stages(size):
    bits = [1 << k for k in range(size.bit_length() - 1)]
    assert size == 1 << len(bits)
    stages = [bits[:1]]
    for k in range(1, len(bits), 2):
        pair = bits[k : k + 2]
        stages.append(pair + [pair[0] ^ pair[1]] if len(pair) == 2 else pair)
    return stages


def gather_bands(x):
    size = lax.axis_size("rows")
    assert size & (size - 1) == 0
    blocks = {0: x}
    hops = [h for h in (1 << k for k in range(size.bit_length() - 1))][::-1]
    for hop in hops:
        pairs = [(i, i ^ hop) for i in range(size)]
        for m in list(blocks):
            blocks[m ^ hop] = lax.ppermute(blocks[m], "rows", pairs)
    return [blocks[m] for m in range(size)]


def on_device(real_frames, fake_frames, *params):
    convs, biases, linears = (params[0:5], params[5:10], params[10:15])
    frames, _, band_rows, width = real_frames.shape
    bands = lax.axis_size("rows")
    frame_total = frames * lax.axis_size("dp")
    work = []
    for n in range(frames):
        c1, c2, b1 = (convs[0], convs[1], biases[0].reshape(1, -1))
        c2 = c2.reshape(9, *c2.shape[2:])
        x, c1, c2, b1 = prep(real_frames[n], fake_frames[n], c1, c2, b1)
        x = gather_bands(x)
        work.append(frame_work(x, c1, c2, b1, convs, biases, linears, band_rows))
    total = functools.reduce(jnp.add, [loss for loss, _ in work])
    axes = ("dp", "rows")
    size = lax.axis_size(axes)
    stages = sum_stages(size)
    states = [None] * frames
    done = 0
    for stage, hops in enumerate(stages):
        others = [lax.ppermute(total, axes, [(i, i ^ hop) for i in range(size)]) for hop in hops]
        last = 5 if stage == len(stages) - 1 else min(5, 1 + 2 * stage)
        for k in range(done, last):
            states = [steps[k](s) for s, (_, steps) in zip(states, work)]
        done = last
        total, others, states = lax.optimization_barrier((total, others, states))
        total = functools.reduce(jnp.add, others, total)
    counts = [frame_total * (band_rows * bands >> s) * (width >> s) for s in range(5)]
    losses = jnp.sum(total, axis=1)[0:5] * jnp.array([1.0 / c for c in counts], F32)
    return (losses, jnp.stack(states))


def solution(mesh):
    frame = P("dp", None, "rows", None)
    return jax.shard_map(
        on_device,
        mesh=mesh,
        in_specs=(frame, frame) + (P(),) * 15,
        out_specs=(P(), frame),
        check_vma=False,
    )
```

```python
import functools
import math

import jax
import jax.numpy as jnp
from jax import lax
from jax.experimental import pallas as pl
from jax.experimental.pallas import tpu as pltpu
from jax.sharding import PartitionSpec as P

EPS = 1e-06
F32 = jnp.float32
BF16 = jnp.bfloat16
K0 = math.sqrt(2.0 / math.pi)
K1 = K0 * 0.044715
PH = 16
LANES = 128
HALF = 64
ONE = (PH + 2) * 3
MIB = 1 << 20
VM = pl.BlockSpec(memory_space=pltpu.VMEM)
HBM = pl.BlockSpec(memory_space=pltpu.HBM)


def gelu(h):
    t = jnp.tanh(h * (2.0 * K0 + (8.0 * K1) * (h * h)))
    return h + h * t


def gelu_back(h):
    sq = h * h
    t = jnp.tanh(h * (2.0 * K0 + (8.0 * K1) * sq))
    return (0.5 + 0.5 * t) + (h * (1.0 - t * t)) * (K0 + (12.0 * K1) * sq)


def dot(a, b):
    return lax.dot_general(a, b, (((1,), (0,)), ((), ())), preferred_element_type=F32)


def dot_t(a, b):
    return lax.dot_general(a, b, (((1,), (1,)), ((), ())), preferred_element_type=F32)


def iota(shape, dim):
    return lax.broadcasted_iota(jnp.int32, shape, dim)


def low_half(shape):
    return iota(shape, len(shape) - 1) % LANES < HALF


def shifted(value, step):
    n, length, chans = value.shape
    flat = value.reshape(n * length, chans)
    place = iota(flat.shape, 0) % length
    if step > 0:
        out = jnp.where(place == 0, 0.0, pltpu.roll(flat, 1, 0))
    else:
        out = jnp.where(place == length - 1, 0.0, pltpu.roll(flat, n * length - 1, 0))
    return out.reshape(n, length, chans)


def call(body, outs, ins, name, scratch=(), limit=16, flops=0, far=()):
    far = [pltpu.with_memory_space_constraint(v, pltpu.HBM) for v in far]
    return pl.pallas_call(
        body,
        out_shape=outs,
        in_specs=[HBM] * len(far) + [VM] * len(ins),
        out_specs=jax.tree.map(lambda _: VM, outs),
        scratch_shapes=scratch,
        name=name,
        cost_estimate=pl.CostEstimate(flops=flops, transcendentals=0, bytes_accessed=0),
        compiler_params=pltpu.CompilerParams(vmem_limit_bytes=limit * MIB),
    )(*far, *ins)


def prep_body(
    real_hbm, fake_hbm, c1_hbm, c2_hbm, b1_hbm,
    out_ref, c1, c2, b1, real_ref, fake_ref, sems,
):
    pairs = ((real_hbm, real_ref), (fake_hbm, fake_ref), (c1_hbm, c1), (c2_hbm, c2), (b1_hbm, b1))
    copies = [pltpu.make_async_copy(a, b, sems.at[i]) for i, (a, b) in enumerate(pairs)]
    for copy in copies:
        copy.start()
    _, rows, width = real_ref.shape
    length = width // PH
    shape = (rows * length, width)
    col = iota(shape, 1)
    place = iota(shape, 0) % length
    inside = col // PH == place
    edges = (col == place * PH - 1) | (col == place * PH + PH)
    eshape = (width, LANES)
    ecol = iota(eshape, 0) % PH
    lane = iota(eshape, 1)
    total = jnp.zeros((rows * length, LANES), F32)
    for copy in copies:
        copy.wait()
    for img, ref in enumerate((real_ref, fake_ref)):
        for ch in range(3):
            x = ref[ch].astype(F32)
            wide = jnp.broadcast_to(x[:, None, :], (rows, length, width)).reshape(shape)
            base = img * HALF + ch
            a = jnp.concatenate(
                [jnp.where(inside, wide, 0.0), jnp.where(edges, wide, 0.0)], axis=1
            ).astype(BF16)
            e_in = lane == base + (ecol + 1) * 3
            e_edge = ((ecol == PH - 1) & (lane == base)) | (
                (ecol == 0) & (lane == base + (PH + 1) * 3)
            )
            e = jnp.concatenate(
                [jnp.where(e_in, 1.0, 0.0), jnp.where(e_edge, 1.0, 0.0)], axis=0
            ).astype(BF16)
            total = total + dot(a, e)
    lane = iota(total.shape, 1) % HALF
    total = jnp.where((lane >= ONE) & (lane < ONE + 3), 1.0, total)
    out_ref[...] = total.astype(BF16).reshape(rows, length, LANES)


def prep(real, fake, c1, c2, b1):
    _, rows, width = real.shape
    V = pltpu.VMEM
    return call(
        prep_body,
        (V((rows, width // PH, LANES), BF16), V(c1.shape, BF16), V(c2.shape, BF16), V(b1.shape, F32)),
        (),
        "prep",
        (V(real.shape, BF16), V(fake.shape, BF16), pltpu.SemaphoreType.DMA((5,))),
        limit=8,
        far=(real, fake, c1, c2, b1),
    )


def weights_body(c1_ref, c2_ref, b1_ref, w1, r1, w2, w2t, base, bias):
    C1, C2 = c2_ref.shape[1:]
    base[...] = jnp.zeros(base.shape, F32)
    for dr in range(3):
        for dc in range(3):
            blk = c1_ref[dr, dc].astype(F32)
            base[dr, dc * 3 : dc * 3 + 3, 0:HALF] = blk
            base[dr, dc * 3 : dc * 3 + 3, HALF:LANES] = blk
    bias[0:1, 0:HALF] = b1_ref[...]
    bias[0:1, HALF:LANES] = b1_ref[...]
    left = bias[0:1, :]
    shape = (HALF, LANES)
    row = iota(shape, 0)
    lo = low_half(shape)
    extra = jnp.zeros(shape, F32)
    for k in range(3):
        part = left.astype(BF16).astype(F32)
        extra = jnp.where(row == ONE + k, jnp.broadcast_to(part, shape), extra)
        left = left - part
    for dr in range(3):
        b = base[dr]
        for i in range(PH // 2):
            first = pltpu.roll(b, (6 * i) % HALF, 0) if i else b
            blk = jnp.where(lo, first, pltpu.roll(b, (6 * i + 3) % HALF, 0))
            if dr == 1:
                blk = blk + extra
            w1[dr * HALF : (dr + 1) * HALF, i * LANES : (i + 1) * LANES] = (0.5 * blk).astype(BF16)
        b = base[2 - dr]
        for j in range(PH // 2 + 2):
            s0, s1 = ((6 * j - 9) % HALF, (6 * j - 6) % HALF)
            blk = jnp.where(
                lo, pltpu.roll(b, s0, 0) if s0 else b, pltpu.roll(b, s1, 0) if s1 else b
            )
            r1[dr * HALF : (dr + 1) * HALF, j * LANES : (j + 1) * LANES] = blk.astype(BF16)
    w1[3 * HALF : 4 * HALF, :] = jnp.zeros((HALF, w1.shape[1]), BF16)
    r1[3 * HALF : 4 * HALF, :] = jnp.zeros((HALF, r1.shape[1]), BF16)
    w2[...] = jnp.zeros(w2.shape, BF16)
    w2t[...] = jnp.zeros(w2t.shape, BF16)
    slot = (2, 0, 1, 3)
    for dr in range(3):
        for dc in range(3):
            blk = c2_ref[dr * 3 + dc]
            back = c2_ref[(2 - dr) * 3 + 2 - dc]
            for u in range(2):
                k = (dr * 4 + slot[dc + u]) * C1
                w2[k : k + C1, u * C2 : (u + 1) * C2] = (blk.astype(F32) * 0.125).astype(BF16)
                k = (dr * 4 + dc + u) * C2
                for d in range(2):
                    n = (u * 2 + d) * C1
                    w2t[n : n + C1, k : k + C2] = back


def three(load):
    return jnp.concatenate([load(dr, dc) for dr in range(3) for dc in range(3)], axis=1)


def pooled_into(ref, img, row, value):
    rows, phases = value.shape[0:2]
    at = pl.ds(row + 1, rows)
    ref[img, at, 1 : phases + 1] = value.astype(BF16)
    ref[img, at, 0] = shifted(value[:, phases - 1], 1).astype(BF16)
    ref[img, at, phases + 1] = shifted(value[:, 0], -1).astype(BF16)


def inverse_norms(r, f, ones2, chans):
    sums = dot(jnp.concatenate([r * r, f * f], axis=1), ones2)
    reps = chans // LANES

    def spread(v):
        return jnp.concatenate([v] * reps, axis=1) if reps > 1 else v

    inv = lax.rsqrt(sums + EPS)
    return spread(inv[:, 0:LANES]), spread(inv[:, LANES : 2 * LANES])


def ones_for(seg, chans):
    rr = iota((2 * chans, 2 * LANES), 0)
    cc = iota((2 * chans, 2 * LANES), 1)
    if seg == 1:
        return jnp.where(rr // HALF == cc // HALF, 1.0, 0.0).astype(BF16)
    return jnp.where(rr // chans == cc // LANES, 1.0, 0.0).astype(BF16)


def forward_body(
    dims,
    *refs,
):
    H, L, HB, C1, C2, C3, C4, C5 = dims
    far, refs = (refs[0:12], refs[12:])
    blocks, refs = (refs[0 : H // HB], refs[H // HB :])
    w1, w2, loss_ref, t1, t2, t3, t4, t5, z1, z2, z3, z4, z5 = refs[0:13]
    near, refs = (refs[13:25], refs[25:])
    w3, w4, w5, b2_ref, b3_ref, b4_ref, b5_ref, *l_refs = near
    xs, xk, p1, p2, p3, p4, a1, a2, a3, a4, a5, sems = refs
    copies = [pltpu.make_async_copy(a, b, sems.at[i]) for i, (a, b) in enumerate(zip(far, near))]
    for copy in copies[3:] + copies[:3]:
        copy.start()
    ph2, ph3, ph4 = (PH // 2, PH // 4, PH // 8)
    band = lax.axis_index("rows")
    for p in (p1, p2, p3, p4):
        n = p.shape[1]
        for img in range(2):
            p[img, 0] = jnp.zeros(p.shape[2:], BF16)
            p[img, n - 1] = jnp.zeros(p.shape[2:], BF16)

    xs[0] = jnp.zeros((L, LANES), BF16)
    xs[H + 1] = jnp.zeros((L, LANES), BF16)
    for m, block in enumerate(blocks):
        xs[pl.ds((band ^ m) * HB + 1, HB)] = block[...]
    x = xs[...].astype(F32)
    xr = pltpu.roll(x.reshape((H + 2) * L, LANES), HALF, 1).reshape(H + 2, L, LANES)
    lo3 = low_half((H, L, LANES))
    xk[0, :, :, 0:LANES] = jnp.where(lo3, x[0:H], xr[1 : H + 1]).astype(BF16)
    xk[0, :, :, LANES : 2 * LANES] = x[2 : H + 2].astype(BF16)
    xk[1, :, :, 0:LANES] = jnp.where(lo3, xr[0:H], x[1 : H + 1]).astype(BF16)
    xk[1, :, :, LANES : 2 * LANES] = xr[2 : H + 2].astype(BF16)

    def keep(r0, rows, size, first):
        place = r0 - first
        return pl.ds(jnp.where((place >= 0) & (place < size), place, size), rows)

    rows = ROWS1

    @pl.loop(0, H // rows, unroll=2)
    def _(step):
        r0 = step * rows
        kept = keep(r0, rows, HB + 2 * rows, band * HB - rows)
        at = pl.ds(r0 // 2 + 1, rows // 2)
        for img in range(2):
            lhs = xk[img, pl.ds(r0, rows)].reshape(rows * L, 2 * LANES)
            for n in range(PH // 4):
                h = dot(lhs, w1[:, n * 256 : (n + 1) * 256])
                act = gelu(h)
                for i in range(2):
                    lanes = slice(i * LANES, (i + 1) * LANES)
                    part = act[:, lanes].reshape(rows, L, LANES)
                    a1[img, pl.ds(r0 + PAD, rows), n * 2 + i] = part.astype(BF16)
                    if img:
                        z1[kept, n * 2 + i] = h[:, lanes].reshape(rows, L, LANES)
                    pair = part.reshape(rows // 2, 2, L, LANES)
                    s = (pair[:, 0] + pair[:, 1]).reshape(rows // 2 * L, LANES)
                    s = (s + pltpu.roll(s, HALF, 1)).reshape(rows // 2, L, LANES)
                    half = slice(i * HALF, (i + 1) * HALF)
                    p1[img, at, n, :, half] = s.astype(BF16)[..., half]
                    q = n * 2 + i
                    other = slice((1 - i) * HALF, (2 - i) * HALF)
                    if q == ph2 - 1:
                        s = shifted(s, 1)
                    if q == 0:
                        s = shifted(s, -1)
                    slot = ph3 + (n + 1 if i else n - 1) % ph3
                    p1[img, at, slot, :, other] = s.astype(BF16)[..., other]

    for copy in copies[3:]:
        copy.wait()

    rows2, rows3, rows4 = (ROWS2, ROWS3, ROWS4)
    loss_ref[...] = jnp.zeros(loss_ref.shape, F32)

    def tap(seg):
        s = seg - 1
        acts = (a1, a2, a3, a4, a5)[s]
        taps(seg, acts, (t1, t2, t3, t4, t5)[s], l_refs[s], loss_ref, HB >> s, band, H // HB)

    for copy in copies[:3]:
        copy.wait()
    tap(1)
    bias = jnp.concatenate([b2_ref[...]] * 2, axis=1) * 0.5

    for step in range(H // 2 // rows2):
        r0 = step * rows2
        kept = keep(r0, rows2, HB // 2 + 2 * rows2, band * (HB // 2) - rows2)
        for img in range(2):
            lhs = jnp.concatenate(
                [
                    p1[img, pl.ds(r0 + dr, rows2), k * ph3 : (k + 1) * ph3].reshape(
                        rows2 * ph3 * L, LANES
                    )
                    for dr in range(3)
                    for k in range(2)
                ],
                axis=1,
            )
            h = dot(lhs, w2[...]) + bias
            act = gelu(h)
            for u in range(2):
                lanes = slice(u * C2, (u + 1) * C2)
                a2[img, pl.ds(r0 + PAD, rows2), u] = act[:, lanes].astype(BF16).reshape(rows2, ph3, L, C2)
                if img:
                    z2[kept, u] = h[:, lanes].reshape(rows2, ph3, L, C2)
            s = (act[:, 0:C2] + act[:, C2 : 2 * C2]).reshape(rows2 // 2, 2, ph3, L, C2)
            pooled_into(p2, img, r0 // 2, (s[:, 0] + s[:, 1]) * 0.125)

    tap(2)
    bias3 = b3_ref[...] * 0.5

    for step in range(H // 4 // rows3):
        r0 = step * rows3
        kept = keep(r0, rows3, HB // 4 + 2 * rows3, band * (HB // 4) - rows3)
        for img in range(2):
            lhs = three(
                lambda dr, dc: p2[img, pl.ds(r0 + dr, rows3), dc : dc + ph3].reshape(
                    rows3 * ph3 * L, C2
                )
            )
            h = dot(lhs, w3[...]) + bias3
            act = gelu(h)
            a3[img, pl.ds(r0 + PAD, rows3)] = act.astype(BF16).reshape(rows3, ph3, L, C3)
            if img:
                z3[kept] = h.reshape(rows3, ph3, L, C3)
            pair = act.reshape(rows3 // 2, 2, ph4, 2, L, C3)
            pooled = (pair[:, 0, :, 0] + pair[:, 0, :, 1]) + (pair[:, 1, :, 0] + pair[:, 1, :, 1])
            pooled_into(p3, img, r0 // 2, pooled * 0.125)

    tap(3)
    bias4 = b4_ref[...] * 0.5

    for step in range(H // 8 // rows4):
        r0 = step * rows4
        lhs = jnp.concatenate(
            [
                three(
                    lambda dr, dc, img=img: p3[
                        img, pl.ds(r0 + dr, rows4), dc : dc + ph4
                    ].reshape(rows4 * ph4 * L, C3)
                )
                for img in range(2)
            ],
            axis=0,
        )
        m = rows4 * ph4 * L
        at = pl.ds(r0 + 2, rows4)
        to = pl.ds(r0 // 2 + 1, rows4 // 2)
        for n in range(0, C4, 256):
            lanes = slice(n, n + 256)
            both = dot(lhs, w4[:, lanes]) + bias4[:, lanes]
            for img in range(2):
                h = both[img * m : (img + 1) * m]
                act = gelu(h)
                a4[img, at, :, :, lanes] = act.astype(BF16).reshape(rows4, ph4, L, 256)
                if img:
                    z4[at, :, :, lanes] = h.reshape(rows4, ph4, L, 256)
                pair = act.reshape(rows4 // 2, 2, ph4, L, 256)
                pooled = (pair[:, 0, 0] + pair[:, 0, 1]) + (pair[:, 1, 0] + pair[:, 1, 1])
                pooled = pooled * 0.125
                p4[img, to, 1, :, lanes] = pooled.astype(BF16)
                p4[img, to, 0, :, lanes] = shifted(pooled, 1).astype(BF16)
                p4[img, to, 2, :, lanes] = shifted(pooled, -1).astype(BF16)

    tap(4)
    h5 = H // 16
    lhs = jnp.concatenate(
        [
            three(lambda dr, dc: p4[img, dr : dr + h5, dc].reshape(h5 * L, C4))
            for img in range(2)
        ],
        axis=0,
    )
    h = dot(lhs, w5[...]) + b5_ref[...] * 0.5
    act = gelu(h).astype(BF16)
    for img in range(2):
        a5[img, 2 : 2 + h5, 0] = act[img * h5 * L : (img + 1) * h5 * L].reshape(h5, L, C5)
    z5[2 : 2 + h5, 0] = h[h5 * L :].reshape(h5, L, C5)
    tap(5)


def taps(seg, acts, grads, l_ref, loss_ref, own, band, bands):
    chans = acts.shape[-1]
    inner = acts.shape[2:-1]
    halo = 1 if seg == 1 else 2
    count = own + 2 * halo
    chunk = TAP_ROWS[seg - 1] or count
    local = band * own - halo + PAD
    m = chunk * math.prod(inner)
    scale = -2.0 * 4.0 ** (seg - 1)
    ones2 = ones_for(seg, chans)
    ones1 = ones2[0:LANES, 0:LANES] if seg == 1 else jnp.ones((chans, LANES), BF16)
    reps = chans // LANES
    lin = l_ref[...]
    if seg == 1:
        lin = jnp.concatenate([lin, lin], axis=1)

    def piece(k):
        i0 = k * chunk
        at = pl.ds(local + i0, chunk)
        r = acts[0, at].reshape(m, chans)
        f = acts[1, at].reshape(m, chans)
        inv_r, inv_f = inverse_norms(r, f, ones2, chans)
        nf = f.astype(F32) * inv_f
        d = r.astype(F32) * inv_r - nf
        ld = lin * d
        q = dot((nf * ld).astype(BF16), ones1)
        if reps > 1:
            q = jnp.concatenate([q] * reps, axis=1)
        tap = (ld - nf * q) * (inv_f * scale)
        grads[pl.ds(i0, chunk)] = tap.reshape((chunk,) + inner + (chans,))
        mapped = (d * d).reshape((chunk,) + inner + (chans,))
        place = iota(mapped.shape, 0) + i0
        mapped = jnp.where((place >= halo) & (place < halo + own), mapped, 0.0)
        add(mapped)

    def add(mapped):
        part = jnp.sum(mapped.reshape(-1, chans), axis=0, keepdims=True) * lin
        acc = part[:, 0:LANES]
        for j in range(1, reps):
            acc = acc + part[:, j * LANES : (j + 1) * LANES]
        loss_ref[seg - 1 : seg, :] += acc

    def other(row, size):
        at = pl.ds(row, size)
        m = size * math.prod(inner)
        r = acts[0, at].reshape(m, chans)
        f = acts[1, at].reshape(m, chans)
        inv_r, inv_f = inverse_norms(r, f, ones2, chans)
        d = r.astype(F32) * inv_r - f.astype(F32) * inv_f
        add(d * d)

    for k in range(count // chunk):
        piece(k)
    size = min(own, OTHER_ROWS[seg - 1])
    for m_ in range(2, bands, 2):
        for k in range(own // size):
            other((band ^ m_) * own + PAD + k * size, size)


def pre_grads(seg, tap_ref, pres, grads, band, HB, H, up, local, halo, chunk):
    chans = pres.shape[-1]
    inner = pres.shape[1:-1]
    own = HB >> (seg - 1)
    total_rows = H >> (seg - 1)
    start = band * own - halo
    shape = (chunk,) + inner + (chans,)

    def piece(k):
        i0 = k * chunk
        g = tap_ref[pl.ds(i0, chunk)]
        if up is not None:
            g = g + up(i0, chunk).reshape(shape)
        g = gelu_back(pres[pl.ds(local + i0, chunk)]) * g
        place = iota(shape, 0) + (start + i0)
        g = jnp.where((place >= 0) & (place < total_rows), g, 0.0)
        to = pl.ds(i0, chunk)
        if seg == 2:
            n = inner[1]
            for u in range(2):
                grads[to, u, 1 : n + 1] = g[:, u].astype(BF16)
            grads[to, 1, 0] = shifted(g[:, 1, n - 1], 1).astype(BF16)
            grads[to, 0, n + 1] = shifted(g[:, 0, 0], -1).astype(BF16)
        else:
            n = inner[0]
            grads[to, 1 : n + 1] = g.astype(BF16)
            grads[to, 0] = shifted(g[:, n - 1], 1).astype(BF16)
            grads[to, n + 1] = shifted(g[:, 0], -1).astype(BF16)

    count = own + 2 * halo
    if count == chunk:
        piece(0)
    else:
        pl.loop(0, count // chunk)(piece)


def back5_body(dims, t5, z5, w5, i5, g5):
    H, L, HB, C1, C2, C3, C4, C5 = dims
    band = lax.axis_index("rows")
    own = HB // 16
    pre_grads(5, t5, z5, g5, band, HB, H, None, band * own, 2, own + 4)
    n = own + 2
    lhs = three(lambda dr, dc: g5[dr : dr + n, dc].reshape(n * L, C5))
    rhs = jnp.concatenate([w5[t * C4 : (t + 1) * C4, :] for t in range(8, -1, -1)], axis=1)
    i5[...] = (dot_t(lhs, rhs) * 0.25).reshape(n, 1, L, C4)


def spread_up(ref, axes):
    def load(i0, chunk):
        v = ref[pl.ds(i0 // 2, chunk // 2)]
        n, ph, length, chans = v.shape
        if axes:
            v = jnp.broadcast_to(v[:, None, None], (n, 2, 2, ph, length, chans))
            return v
        return jnp.broadcast_to(v[:, None, :, None], (n, 2, ph, 2, length, chans))

    return load


def back4_body(dims, t4, z4, w4, i5, i4, g4):
    H, L, HB, C1, C2, C3, C4, C5 = dims
    band = lax.axis_index("rows")
    own, ph = (HB // 8, PH // 8)
    pre_grads(4, t4, z4, g4, band, HB, H, spread_up(i5, 0), band * own, 2, own + 4)
    n = own + 2
    lhs = three(lambda dr, dc: g4[dr : dr + n, dc : dc + ph].reshape(n * ph * L, C4))
    rhs = jnp.concatenate([w4[t * C3 : (t + 1) * C3, :] for t in range(8, -1, -1)], axis=1)
    i4[...] = (dot_t(lhs, rhs) * 0.25).reshape(n, ph, L, C3)


def back3_body(dims, t3, z3, w3, i4, i3, g3):
    H, L, HB, C1, C2, C3, C4, C5 = dims
    band = lax.axis_index("rows")
    own, ph = (HB // 4, PH // 4)
    pre_grads(3, t3, z3, g3, band, HB, H, spread_up(i4, 0), ROWS3 - 2, 2, own + 4)
    n = own + 2
    lhs = three(lambda dr, dc: g3[dr : dr + n, dc : dc + ph].reshape(n * ph * L, C3))
    rhs = jnp.concatenate([w3[t * C2 : (t + 1) * C2, :] for t in range(8, -1, -1)], axis=1)
    i3[...] = (dot_t(lhs, rhs) * 0.25).reshape(n, ph, L, C2)


def back2_body(dims, t2, z2, w2t, i3, i2, g2):
    H, L, HB, C1, C2, C3, C4, C5 = dims
    band = lax.axis_index("rows")
    own, ph = (HB // 2, PH // 4)
    pre_grads(2, t2, z2, g2, band, HB, H, spread_up(i3, 1), ROWS2 - 2, 2, 6)
    step = (own + 2) // 2
    for r0 in (0, step):
        lhs = jnp.concatenate(
            [
                g2[r0 + dr : r0 + dr + step, 1 - j % 2, (j + 1) // 2 : (j + 1) // 2 + ph].reshape(
                    step * ph * L, C2
                )
                for dr in range(3)
                for j in range(4)
            ],
            axis=1,
        )
        out = (dot_t(lhs, w2t[...]) * 0.25).reshape(step, ph, L, 2 * LANES)
        for u in range(2):
            i2[r0 : r0 + step, u] = out[..., u * LANES : (u + 1) * LANES]


def back1_body(dims, t1, z1, r1, i2, grad_ref, g1):
    H, L, HB, C1, C2, C3, C4, C5 = dims
    band = lax.axis_index("rows")
    ph = PH // 4

    def up(i0, chunk):
        v = i2[pl.ds(i0 // 2, chunk // 2 + 1)]
        v = jnp.stack([v[:, q % 2, q // 2] for q in range(2 * ph)], axis=1)
        return jnp.stack([v[(j + 1) // 2] for j in range(chunk)])

    pre_grads(1, t1, z1, g1, band, HB, H, up, ROWS1 - 1, 1, 6)
    lhs = jnp.concatenate(
        [g1[:, j].reshape((HB + 2) * L, LANES) for j in range(PH // 2 + 2)], axis=1
    )
    rows3 = dot_t(lhs, r1[...]).reshape(HB + 2, L, 2 * LANES)
    first = rows3[0:HB, :, 0:LANES].reshape(HB * L, LANES)
    second = rows3[1 : HB + 1, :, 0:LANES].reshape(HB * L, LANES)
    third = rows3[2 : HB + 2, :, LANES : 2 * LANES].reshape(HB * L, LANES)
    gin = (first + pltpu.roll(second, HALF, 1) + third)[:, 0:HALF]
    high = gin.astype(BF16)
    split = jnp.concatenate([high.astype(F32), gin - high.astype(F32)], axis=1).astype(BF16)
    width = PH * L
    sel_row = iota((LANES, width), 0) % HALF
    sel_col = iota((LANES, width), 1) % PH
    shape = (HB * L, width)
    inside = iota(shape, 1) // PH == iota(shape, 0) % L
    for ch in range(3):
        pick = jnp.where(sel_row == sel_col * 3 + ch, 1.0, 0.0).astype(BF16)
        wide = jnp.where(inside, dot(split, pick), 0.0)
        grad_ref[ch] = jnp.sum(wide.reshape(HB, L, width), axis=1)


ROWS1, ROWS2, ROWS3, ROWS4 = (8, 4, 4, 8)
TAP_ROWS = (6, 4, 4, 0, 0)
OTHER_ROWS = (4, 4, 4, 2, 1)
PAD = 2


def frame_work(x, c1, c2, b1, convs, biases, linears, HB):
    H, L, _ = x[0].shape
    H = H * len(x)
    C1, C2, C3, C4, C5 = [c.shape[-1] for c in convs]
    dims = (H, L, HB, C1, C2, C3, C4, C5)
    ph2, ph3, ph4 = (PH // 2, PH // 4, PH // 8)
    V = pltpu.VMEM
    far = [c.reshape(-1, c.shape[-1]) for c in convs[2:]]
    far += [v.reshape(1, -1) for v in (*biases[1:], *linears)]
    w1, r1, w2, w2t = call(
        weights_body,
        (
            V((4 * HALF, PH * HALF), BF16),
            V((4 * HALF, (ph2 + 2) * LANES), BF16),
            V((12 * C1, 2 * C2), BF16),
            V((4 * C1, 12 * C2), BF16),
        ),
        (c1, c2, b1),
        "weights",
        (V((3, HALF, LANES), F32), V((8, LANES), F32)),
        limit=8,
    )
    acts = (
        (HB + 3 * ROWS1, ph2, L, LANES),
        (HB // 2 + 3 * ROWS2, 2, ph3, L, C2),
        (HB // 4 + 3 * ROWS3, ph3, L, C3),
        (H // 8 + 4, ph4, L, C4),
        (H // 16 + 4, 1, L, C5),
    )
    outs = (V((8, LANES), F32),)
    halos = (1, 2, 2, 2, 2)
    outs += tuple(V(((HB >> i) + 2 * halos[i],) + s[1:], F32) for i, s in enumerate(acts))
    outs += tuple(V(s, F32) for s in acts)
    outs += tuple(V(v.shape, v.dtype) for v in far)
    loss, t1, t2, t3, t4, t5, z1, z2, z3, z4, z5, w3, w4, w5, *_ = call(
        functools.partial(forward_body, dims),
        outs,
        (*x, w1, w2),
        "forward",
        (
            V((H + 2, L, LANES), BF16),
            V((2, H, L, 2 * LANES), BF16),
            V((2, H // 2 + 2, ph2, L, LANES), BF16),
            V((2, H // 4 + 2, ph3 + 2, L, C2), BF16),
            V((2, H // 8 + 2, ph4 + 2, L, C3), BF16),
            V((2, H // 16 + 2, 3, L, C4), BF16),
            *[V((2, (H >> i) + 2 * PAD) + s[1:], BF16) for i, s in enumerate(acts)],
            pltpu.SemaphoreType.DMA((12,)),
        ),
        limit=32,
        far=far,
    )
    n1, n2, n3, n4, n5 = (HB + 2, HB // 2 + 4, HB // 4 + 4, HB // 8 + 4, HB // 16 + 4)

    def step(body, name, ins, out, scratch, flops):
        return call(functools.partial(body, dims), out, ins, name, (V(scratch, BF16),), 12, flops)

    def back5(_):
        return step(
            back5_body, "back5", (t5, z5, w5), V((n5 - 2, 1, L, C4), F32), (n5, 3, L, C5), FL
        )

    def back4(i5):
        return step(
            back4_body, "back4", (t4, z4, w4, i5), V((n4 - 2, ph4, L, C3), F32),
            (n4, ph4 + 2, L, C4), FL,
        )

    def back3(i4):
        return step(
            back3_body, "back3", (t3, z3, w3, i4), V((n3 - 2, ph3, L, C2), F32),
            (n3, ph3 + 2, L, C3), FL,
        )

    def back2(i3):
        return step(
            back2_body, "back2", (t2, z2, w2t, i3), V((n2 - 2, 2, ph3, L, LANES), F32),
            (n2, 2, ph3 + 2, L, C2), FL,
        )

    def back1(i2):
        return step(
            back1_body, "back1", (t1, z1, r1, i2),
            jax.ShapeDtypeStruct((3, HB, L * PH), F32), (n1, ph2 + 2, L, LANES), FL,
        )

    return loss, (back5, back4, back3, back2, back1)


FL = 10**9


def gather_bands(x):
    size = lax.axis_size("rows")
    assert size & (size - 1) == 0
    blocks = {0: x}
    hops = [h for h in (1 << k for k in range(size.bit_length() - 1))][::-1]
    for hop in hops:
        pairs = [(i, i ^ hop) for i in range(size)]
        for m in list(blocks):
            blocks[m ^ hop] = lax.ppermute(blocks[m], "rows", pairs)
    return [blocks[m] for m in range(size)]


def on_device(real_frames, fake_frames, *params):
    convs, biases, linears = (params[0:5], params[5:10], params[10:15])
    frames, _, band_rows, width = real_frames.shape
    bands = lax.axis_size("rows")
    frame_total = frames * lax.axis_size("dp")
    work = []
    for n in range(frames):
        c1, c2, b1 = (convs[0], convs[1], biases[0].reshape(1, -1))
        c2 = c2.reshape(9, *c2.shape[2:])
        x, c1, c2, b1 = prep(real_frames[n], fake_frames[n], c1, c2, b1)
        x = gather_bands(x)
        work.append(frame_work(x, c1, c2, b1, convs, biases, linears, band_rows))
    total = functools.reduce(jnp.add, [loss for loss, _ in work])
    hops = [("rows", 1)]
    size = lax.axis_size("dp")
    hops += [("dp", 1 << k) for k in range(size.bit_length() - 1)]
    assert size == 1 << len(hops) - 1
    states = [None] * frames
    done = 0
    for stage, (axis, hop) in enumerate(hops):
        pairs = [(i, i ^ hop) for i in range(lax.axis_size(axis))]
        other = lax.ppermute(total, axis, pairs)
        last = 5 if stage == len(hops) - 1 else (1, 3, 4)[min(stage, 2)]
        for k in range(done, last):
            states = [steps[k](s) for s, (_, steps) in zip(states, work)]
        done = last
        total, other, states = lax.optimization_barrier((total, other, states))
        total = total + other
    counts = [frame_total * (band_rows * bands >> s) * (width >> s) for s in range(5)]
    losses = jnp.sum(total, axis=1)[0:5] * jnp.array([1.0 / c for c in counts], F32)
    return (losses, jnp.stack(states))


def solution(mesh):
    frame = P("dp", None, "rows", None)
    return jax.shard_map(
        on_device,
        mesh=mesh,
        in_specs=(frame, frame) + (P(),) * 15,
        out_specs=(P(), frame),
        check_vma=False,
    )
```

```python
import functools
import math

import jax
import jax.numpy as jnp
from jax import lax
from jax.experimental import pallas as pl
from jax.experimental.pallas import tpu as pltpu
from jax.sharding import PartitionSpec as P

EPS = 1e-06
F32 = jnp.float32
BF16 = jnp.bfloat16
K0 = math.sqrt(2.0 / math.pi)
K1 = K0 * 0.044715
PH = 16
LANES = 128
HALF = 64
ONE = (PH + 2) * 3
MIB = 1 << 20
VM = pl.BlockSpec(memory_space=pltpu.VMEM)
HBM = pl.BlockSpec(memory_space=pltpu.HBM)


def gelu(h):
    t = jnp.tanh(h * (2.0 * K0 + (8.0 * K1) * (h * h)))
    return h + h * t


def gelu_back(h):
    sq = h * h
    t = jnp.tanh(h * (2.0 * K0 + (8.0 * K1) * sq))
    return (0.5 + 0.5 * t) + (h * (1.0 - t * t)) * (K0 + (12.0 * K1) * sq)


def dot(a, b):
    return lax.dot_general(a, b, (((1,), (0,)), ((), ())), preferred_element_type=F32)


def dot_t(a, b):
    return lax.dot_general(a, b, (((1,), (1,)), ((), ())), preferred_element_type=F32)


def iota(shape, dim):
    return lax.broadcasted_iota(jnp.int32, shape, dim)


def low_half(shape):
    return iota(shape, len(shape) - 1) % LANES < HALF


def shifted(value, step):
    n, length, chans = value.shape
    flat = value.reshape(n * length, chans)
    place = iota(flat.shape, 0) % length
    if step > 0:
        out = jnp.where(place == 0, 0.0, pltpu.roll(flat, 1, 0))
    else:
        out = jnp.where(place == length - 1, 0.0, pltpu.roll(flat, n * length - 1, 0))
    return out.reshape(n, length, chans)


def call(body, outs, ins, name, scratch=(), limit=16, flops=0, far=()):
    far = [pltpu.with_memory_space_constraint(v, pltpu.HBM) for v in far]
    return pl.pallas_call(
        body,
        out_shape=outs,
        in_specs=[HBM] * len(far) + [VM] * len(ins),
        out_specs=jax.tree.map(lambda _: VM, outs),
        scratch_shapes=scratch,
        name=name,
        cost_estimate=pl.CostEstimate(flops=flops, transcendentals=0, bytes_accessed=0),
        compiler_params=pltpu.CompilerParams(vmem_limit_bytes=limit * MIB),
    )(*far, *ins)


def prep_body(
    real_hbm, fake_hbm, c1_hbm, c2_hbm, b1_hbm,
    out_ref, c1, c2, b1, real_ref, fake_ref, sems,
):
    pairs = ((real_hbm, real_ref), (fake_hbm, fake_ref), (c1_hbm, c1), (c2_hbm, c2), (b1_hbm, b1))
    copies = [pltpu.make_async_copy(a, b, sems.at[i]) for i, (a, b) in enumerate(pairs)]
    for copy in copies:
        copy.start()
    _, rows, width = real_ref.shape
    length = width // PH
    shape = (rows * length, width)
    col = iota(shape, 1)
    place = iota(shape, 0) % length
    inside = col // PH == place
    edges = (col == place * PH - 1) | (col == place * PH + PH)
    eshape = (width, LANES)
    ecol = iota(eshape, 0) % PH
    lane = iota(eshape, 1)
    total = jnp.zeros((rows * length, LANES), F32)
    for copy in copies:
        copy.wait()
    for img, ref in enumerate((real_ref, fake_ref)):
        for ch in range(3):
            x = ref[ch].astype(F32)
            wide = jnp.broadcast_to(x[:, None, :], (rows, length, width)).reshape(shape)
            base = img * HALF + ch
            a = jnp.concatenate(
                [jnp.where(inside, wide, 0.0), jnp.where(edges, wide, 0.0)], axis=1
            ).astype(BF16)
            e_in = lane == base + (ecol + 1) * 3
            e_edge = ((ecol == PH - 1) & (lane == base)) | (
                (ecol == 0) & (lane == base + (PH + 1) * 3)
            )
            e = jnp.concatenate(
                [jnp.where(e_in, 1.0, 0.0), jnp.where(e_edge, 1.0, 0.0)], axis=0
            ).astype(BF16)
            total = total + dot(a, e)
    lane = iota(total.shape, 1) % HALF
    total = jnp.where((lane >= ONE) & (lane < ONE + 3), 1.0, total)
    out_ref[...] = total.astype(BF16).reshape(rows, length, LANES)


def prep(real, fake, c1, c2, b1):
    _, rows, width = real.shape
    V = pltpu.VMEM
    return call(
        prep_body,
        (V((rows, width // PH, LANES), BF16), V(c1.shape, BF16), V(c2.shape, BF16), V(b1.shape, F32)),
        (),
        "prep",
        (V(real.shape, BF16), V(fake.shape, BF16), pltpu.SemaphoreType.DMA((5,))),
        limit=8,
        far=(real, fake, c1, c2, b1),
    )


def weights_body(c1_ref, c2_ref, b1_ref, w1, r1, w2, w2t, base, bias):
    C1, C2 = c2_ref.shape[1:]
    base[...] = jnp.zeros(base.shape, F32)
    for dr in range(3):
        for dc in range(3):
            blk = c1_ref[dr, dc].astype(F32)
            base[dr, dc * 3 : dc * 3 + 3, 0:HALF] = blk
            base[dr, dc * 3 : dc * 3 + 3, HALF:LANES] = blk
    bias[0:1, 0:HALF] = b1_ref[...]
    bias[0:1, HALF:LANES] = b1_ref[...]
    left = bias[0:1, :]
    shape = (HALF, LANES)
    row = iota(shape, 0)
    lo = low_half(shape)
    extra = jnp.zeros(shape, F32)
    for k in range(3):
        part = left.astype(BF16).astype(F32)
        extra = jnp.where(row == ONE + k, jnp.broadcast_to(part, shape), extra)
        left = left - part
    for dr in range(3):
        b = base[dr]
        for i in range(PH // 2):
            first = pltpu.roll(b, (6 * i) % HALF, 0) if i else b
            blk = jnp.where(lo, first, pltpu.roll(b, (6 * i + 3) % HALF, 0))
            if dr == 1:
                blk = blk + extra
            w1[dr * HALF : (dr + 1) * HALF, i * LANES : (i + 1) * LANES] = (0.5 * blk).astype(BF16)
        b = base[2 - dr]
        for j in range(PH // 2 + 2):
            s0, s1 = ((6 * j - 9) % HALF, (6 * j - 6) % HALF)
            blk = jnp.where(
                lo, pltpu.roll(b, s0, 0) if s0 else b, pltpu.roll(b, s1, 0) if s1 else b
            )
            r1[dr * HALF : (dr + 1) * HALF, j * LANES : (j + 1) * LANES] = blk.astype(BF16)
    w1[3 * HALF : 4 * HALF, :] = jnp.zeros((HALF, w1.shape[1]), BF16)
    r1[3 * HALF : 4 * HALF, :] = jnp.zeros((HALF, r1.shape[1]), BF16)
    w2[...] = jnp.zeros(w2.shape, BF16)
    w2t[...] = jnp.zeros(w2t.shape, BF16)
    slot = (2, 0, 1, 3)
    for dr in range(3):
        for dc in range(3):
            blk = c2_ref[dr * 3 + dc]
            back = c2_ref[(2 - dr) * 3 + 2 - dc]
            for u in range(2):
                k = (dr * 4 + slot[dc + u]) * C1
                w2[k : k + C1, u * C2 : (u + 1) * C2] = (blk.astype(F32) * 0.125).astype(BF16)
                k = (dr * 4 + dc + u) * C2
                for d in range(2):
                    n = (u * 2 + d) * C1
                    w2t[n : n + C1, k : k + C2] = back


def three(load):
    return jnp.concatenate([load(dr, dc) for dr in range(3) for dc in range(3)], axis=1)


def pooled_into(ref, img, row, value):
    rows, phases = value.shape[0:2]
    at = pl.ds(row + 1, rows)
    ref[img, at, 1 : phases + 1] = value.astype(BF16)
    ref[img, at, 0] = shifted(value[:, phases - 1], 1).astype(BF16)
    ref[img, at, phases + 1] = shifted(value[:, 0], -1).astype(BF16)


def inverse_norms(r, f, ones2, chans):
    sums = dot(jnp.concatenate([r * r, f * f], axis=1), ones2)
    reps = chans // LANES

    def spread(v):
        return jnp.concatenate([v] * reps, axis=1) if reps > 1 else v

    inv = lax.rsqrt(sums + EPS)
    return spread(inv[:, 0:LANES]), spread(inv[:, LANES : 2 * LANES])


def ones_for(seg, chans):
    rr = iota((2 * chans, 2 * LANES), 0)
    cc = iota((2 * chans, 2 * LANES), 1)
    if seg == 1:
        return jnp.where(rr // HALF == cc // HALF, 1.0, 0.0).astype(BF16)
    return jnp.where(rr // chans == cc // LANES, 1.0, 0.0).astype(BF16)


def forward_body(
    dims,
    *refs,
):
    H, L, HB, C1, C2, C3, C4, C5 = dims
    far, refs = (refs[0:12], refs[12:])
    blocks, refs = (refs[0 : H // HB], refs[H // HB :])
    w1, w2, loss_ref, t1, t2, t3, t4, t5, z1, z2, z3, z4, z5 = refs[0:13]
    near, refs = (refs[13:25], refs[25:])
    w3, w4, w5, b2_ref, b3_ref, b4_ref, b5_ref, *l_refs = near
    xs, xk, p1, p2, p3, p4, a1, a2, a3, a4, a5, sems = refs
    copies = [pltpu.make_async_copy(a, b, sems.at[i]) for i, (a, b) in enumerate(zip(far, near))]
    for copy in copies[3:] + copies[:3]:
        copy.start()
    ph2, ph3, ph4 = (PH // 2, PH // 4, PH // 8)
    band = lax.axis_index("rows")
    for p in (p1, p2, p3, p4):
        n = p.shape[1]
        for img in range(2):
            p[img, 0] = jnp.zeros(p.shape[2:], BF16)
            p[img, n - 1] = jnp.zeros(p.shape[2:], BF16)

    xs[0] = jnp.zeros((L, LANES), BF16)
    xs[H + 1] = jnp.zeros((L, LANES), BF16)
    for m, block in enumerate(blocks):
        xs[pl.ds((band ^ m) * HB + 1, HB)] = block[...]
    x = xs[...].astype(F32)
    xr = pltpu.roll(x.reshape((H + 2) * L, LANES), HALF, 1).reshape(H + 2, L, LANES)
    lo3 = low_half((H, L, LANES))
    xk[0, :, :, 0:LANES] = jnp.where(lo3, x[0:H], xr[1 : H + 1]).astype(BF16)
    xk[0, :, :, LANES : 2 * LANES] = x[2 : H + 2].astype(BF16)
    xk[1, :, :, 0:LANES] = jnp.where(lo3, xr[0:H], x[1 : H + 1]).astype(BF16)
    xk[1, :, :, LANES : 2 * LANES] = xr[2 : H + 2].astype(BF16)

    def keep(r0, rows, size, first):
        place = r0 - first
        return pl.ds(jnp.where((place >= 0) & (place < size), place, size), rows)

    rows = ROWS1

    @pl.loop(0, H // rows, unroll=4)
    def _(step):
        r0 = step * rows
        kept = keep(r0, rows, HB + 2 * rows, band * HB - rows)
        at = pl.ds(r0 // 2 + 1, rows // 2)
        for img in range(2):
            lhs = xk[img, pl.ds(r0, rows)].reshape(rows * L, 2 * LANES)
            for n in range(PH // 4):
                h = dot(lhs, w1[:, n * 256 : (n + 1) * 256])
                act = gelu(h)
                for i in range(2):
                    lanes = slice(i * LANES, (i + 1) * LANES)
                    part = act[:, lanes].reshape(rows, L, LANES)
                    a1[img, pl.ds(r0 + PAD, rows), n * 2 + i] = part.astype(BF16)
                    if img:
                        z1[kept, n * 2 + i] = h[:, lanes].reshape(rows, L, LANES)
                    pair = part.reshape(rows // 2, 2, L, LANES)
                    s = (pair[:, 0] + pair[:, 1]).reshape(rows // 2 * L, LANES)
                    s = (s + pltpu.roll(s, HALF, 1)).reshape(rows // 2, L, LANES)
                    half = slice(i * HALF, (i + 1) * HALF)
                    p1[img, at, n, :, half] = s.astype(BF16)[..., half]
                    q = n * 2 + i
                    other = slice((1 - i) * HALF, (2 - i) * HALF)
                    if q == ph2 - 1:
                        s = shifted(s, 1)
                    if q == 0:
                        s = shifted(s, -1)
                    slot = ph3 + (n + 1 if i else n - 1) % ph3
                    p1[img, at, slot, :, other] = s.astype(BF16)[..., other]

    for copy in copies[3:]:
        copy.wait()

    rows2, rows3, rows4 = (ROWS2, ROWS3, ROWS4)
    loss_ref[...] = jnp.zeros(loss_ref.shape, F32)

    def tap(seg):
        s = seg - 1
        acts = (a1, a2, a3, a4, a5)[s]
        taps(seg, acts, (t1, t2, t3, t4, t5)[s], l_refs[s], loss_ref, HB >> s, band, H // HB)

    for copy in copies[:3]:
        copy.wait()
    tap(1)
    bias = jnp.concatenate([b2_ref[...]] * 2, axis=1) * 0.5

    for step in range(H // 2 // rows2):
        r0 = step * rows2
        kept = keep(r0, rows2, HB // 2 + 2 * rows2, band * (HB // 2) - rows2)
        for img in range(2):
            lhs = jnp.concatenate(
                [
                    p1[img, pl.ds(r0 + dr, rows2), k * ph3 : (k + 1) * ph3].reshape(
                        rows2 * ph3 * L, LANES
                    )
                    for dr in range(3)
                    for k in range(2)
                ],
                axis=1,
            )
            h = dot(lhs, w2[...]) + bias
            act = gelu(h)
            for u in range(2):
                lanes = slice(u * C2, (u + 1) * C2)
                a2[img, pl.ds(r0 + PAD, rows2), u] = act[:, lanes].astype(BF16).reshape(rows2, ph3, L, C2)
                if img:
                    z2[kept, u] = h[:, lanes].reshape(rows2, ph3, L, C2)
            s = (act[:, 0:C2] + act[:, C2 : 2 * C2]).reshape(rows2 // 2, 2, ph3, L, C2)
            pooled_into(p2, img, r0 // 2, (s[:, 0] + s[:, 1]) * 0.125)

    tap(2)
    bias3 = b3_ref[...] * 0.5

    for step in range(H // 4 // rows3):
        r0 = step * rows3
        kept = keep(r0, rows3, HB // 4 + 2 * rows3, band * (HB // 4) - rows3)
        for img in range(2):
            lhs = three(
                lambda dr, dc: p2[img, pl.ds(r0 + dr, rows3), dc : dc + ph3].reshape(
                    rows3 * ph3 * L, C2
                )
            )
            h = dot(lhs, w3[...]) + bias3
            act = gelu(h)
            a3[img, pl.ds(r0 + PAD, rows3)] = act.astype(BF16).reshape(rows3, ph3, L, C3)
            if img:
                z3[kept] = h.reshape(rows3, ph3, L, C3)
            pair = act.reshape(rows3 // 2, 2, ph4, 2, L, C3)
            pooled = (pair[:, 0, :, 0] + pair[:, 0, :, 1]) + (pair[:, 1, :, 0] + pair[:, 1, :, 1])
            pooled_into(p3, img, r0 // 2, pooled * 0.125)

    tap(3)
    bias4 = b4_ref[...] * 0.5

    for step in range(H // 8 // rows4):
        r0 = step * rows4
        lhs = jnp.concatenate(
            [
                three(
                    lambda dr, dc, img=img: p3[
                        img, pl.ds(r0 + dr, rows4), dc : dc + ph4
                    ].reshape(rows4 * ph4 * L, C3)
                )
                for img in range(2)
            ],
            axis=0,
        )
        m = rows4 * ph4 * L
        at = pl.ds(r0 + 2, rows4)
        to = pl.ds(r0 // 2 + 1, rows4 // 2)
        for n in range(0, C4, 256):
            lanes = slice(n, n + 256)
            both = dot(lhs, w4[:, lanes]) + bias4[:, lanes]
            for img in range(2):
                h = both[img * m : (img + 1) * m]
                act = gelu(h)
                a4[img, at, :, :, lanes] = act.astype(BF16).reshape(rows4, ph4, L, 256)
                if img:
                    z4[at, :, :, lanes] = h.reshape(rows4, ph4, L, 256)
                pair = act.reshape(rows4 // 2, 2, ph4, L, 256)
                pooled = (pair[:, 0, 0] + pair[:, 0, 1]) + (pair[:, 1, 0] + pair[:, 1, 1])
                pooled = pooled * 0.125
                p4[img, to, 1, :, lanes] = pooled.astype(BF16)
                p4[img, to, 0, :, lanes] = shifted(pooled, 1).astype(BF16)
                p4[img, to, 2, :, lanes] = shifted(pooled, -1).astype(BF16)

    tap(4)
    h5 = H // 16
    lhs = jnp.concatenate(
        [
            three(lambda dr, dc: p4[img, dr : dr + h5, dc].reshape(h5 * L, C4))
            for img in range(2)
        ],
        axis=0,
    )
    h = dot(lhs, w5[...]) + b5_ref[...] * 0.5
    act = gelu(h).astype(BF16)
    for img in range(2):
        a5[img, 2 : 2 + h5, 0] = act[img * h5 * L : (img + 1) * h5 * L].reshape(h5, L, C5)
    z5[2 : 2 + h5, 0] = h[h5 * L :].reshape(h5, L, C5)
    tap(5)


def taps(seg, acts, grads, l_ref, loss_ref, own, band, bands):
    chans = acts.shape[-1]
    inner = acts.shape[2:-1]
    halo = 1 if seg == 1 else 2
    count = own + 2 * halo
    chunk = TAP_ROWS[seg - 1] or count
    local = band * own - halo + PAD
    m = chunk * math.prod(inner)
    scale = -2.0 * 4.0 ** (seg - 1)
    ones2 = ones_for(seg, chans)
    ones1 = ones2[0:LANES, 0:LANES] if seg == 1 else jnp.ones((chans, LANES), BF16)
    reps = chans // LANES
    lin = l_ref[...]
    if seg == 1:
        lin = jnp.concatenate([lin, lin], axis=1)

    def piece(k):
        i0 = k * chunk
        at = pl.ds(local + i0, chunk)
        r = acts[0, at].reshape(m, chans)
        f = acts[1, at].reshape(m, chans)
        inv_r, inv_f = inverse_norms(r, f, ones2, chans)
        nf = f.astype(F32) * inv_f
        d = r.astype(F32) * inv_r - nf
        ld = lin * d
        q = dot((nf * ld).astype(BF16), ones1)
        if reps > 1:
            q = jnp.concatenate([q] * reps, axis=1)
        tap = (ld - nf * q) * (inv_f * scale)
        grads[pl.ds(i0, chunk)] = tap.reshape((chunk,) + inner + (chans,))
        mapped = (d * d).reshape((chunk,) + inner + (chans,))
        place = iota(mapped.shape, 0) + i0
        mapped = jnp.where((place >= halo) & (place < halo + own), mapped, 0.0)
        add(mapped)

    def add(mapped):
        part = jnp.sum(mapped.reshape(-1, chans), axis=0, keepdims=True) * lin
        acc = part[:, 0:LANES]
        for j in range(1, reps):
            acc = acc + part[:, j * LANES : (j + 1) * LANES]
        loss_ref[seg - 1 : seg, :] += acc

    def other(row, size):
        at = pl.ds(row, size)
        m = size * math.prod(inner)
        r = acts[0, at].reshape(m, chans)
        f = acts[1, at].reshape(m, chans)
        inv_r, inv_f = inverse_norms(r, f, ones2, chans)
        d = r.astype(F32) * inv_r - f.astype(F32) * inv_f
        add(d * d)

    for k in range(count // chunk):
        piece(k)
    size = min(own, OTHER_ROWS[seg - 1])
    for m_ in range(2, bands, 2):
        for k in range(own // size):
            other((band ^ m_) * own + PAD + k * size, size)


def pre_grads(seg, tap_ref, pres, grads, band, HB, H, up, local, halo, chunk):
    chans = pres.shape[-1]
    inner = pres.shape[1:-1]
    own = HB >> (seg - 1)
    total_rows = H >> (seg - 1)
    start = band * own - halo
    shape = (chunk,) + inner + (chans,)

    def piece(k):
        i0 = k * chunk
        g = tap_ref[pl.ds(i0, chunk)]
        if up is not None:
            g = g + up(i0, chunk).reshape(shape)
        g = gelu_back(pres[pl.ds(local + i0, chunk)]) * g
        place = iota(shape, 0) + (start + i0)
        g = jnp.where((place >= 0) & (place < total_rows), g, 0.0)
        to = pl.ds(i0, chunk)
        if seg == 2:
            n = inner[1]
            for u in range(2):
                grads[to, u, 1 : n + 1] = g[:, u].astype(BF16)
            grads[to, 1, 0] = shifted(g[:, 1, n - 1], 1).astype(BF16)
            grads[to, 0, n + 1] = shifted(g[:, 0, 0], -1).astype(BF16)
        else:
            n = inner[0]
            grads[to, 1 : n + 1] = g.astype(BF16)
            grads[to, 0] = shifted(g[:, n - 1], 1).astype(BF16)
            grads[to, n + 1] = shifted(g[:, 0], -1).astype(BF16)

    count = own + 2 * halo
    if count == chunk:
        piece(0)
    else:
        pl.loop(0, count // chunk)(piece)


def back5_body(dims, t5, z5, w5, i5, g5):
    H, L, HB, C1, C2, C3, C4, C5 = dims
    band = lax.axis_index("rows")
    own = HB // 16
    pre_grads(5, t5, z5, g5, band, HB, H, None, band * own, 2, own + 4)
    n = own + 2
    lhs = three(lambda dr, dc: g5[dr : dr + n, dc].reshape(n * L, C5))
    rhs = jnp.concatenate([w5[t * C4 : (t + 1) * C4, :] for t in range(8, -1, -1)], axis=1)
    i5[...] = (dot_t(lhs, rhs) * 0.25).reshape(n, 1, L, C4)


def spread_up(ref, axes):
    def load(i0, chunk):
        v = ref[pl.ds(i0 // 2, chunk // 2)]
        n, ph, length, chans = v.shape
        if axes:
            v = jnp.broadcast_to(v[:, None, None], (n, 2, 2, ph, length, chans))
            return v
        return jnp.broadcast_to(v[:, None, :, None], (n, 2, ph, 2, length, chans))

    return load


def back4_body(dims, t4, z4, w4, i5, i4, g4):
    H, L, HB, C1, C2, C3, C4, C5 = dims
    band = lax.axis_index("rows")
    own, ph = (HB // 8, PH // 8)
    pre_grads(4, t4, z4, g4, band, HB, H, spread_up(i5, 0), band * own, 2, own + 4)
    n = own + 2
    lhs = three(lambda dr, dc: g4[dr : dr + n, dc : dc + ph].reshape(n * ph * L, C4))
    rhs = jnp.concatenate([w4[t * C3 : (t + 1) * C3, :] for t in range(8, -1, -1)], axis=1)
    i4[...] = (dot_t(lhs, rhs) * 0.25).reshape(n, ph, L, C3)


def back3_body(dims, t3, z3, w3, i4, i3, g3):
    H, L, HB, C1, C2, C3, C4, C5 = dims
    band = lax.axis_index("rows")
    own, ph = (HB // 4, PH // 4)
    pre_grads(3, t3, z3, g3, band, HB, H, spread_up(i4, 0), ROWS3 - 2, 2, own + 4)
    n = own + 2
    lhs = three(lambda dr, dc: g3[dr : dr + n, dc : dc + ph].reshape(n * ph * L, C3))
    rhs = jnp.concatenate([w3[t * C2 : (t + 1) * C2, :] for t in range(8, -1, -1)], axis=1)
    i3[...] = (dot_t(lhs, rhs) * 0.25).reshape(n, ph, L, C2)


def back2_body(dims, t2, z2, w2t, i3, i2, g2):
    H, L, HB, C1, C2, C3, C4, C5 = dims
    band = lax.axis_index("rows")
    own, ph = (HB // 2, PH // 4)
    pre_grads(2, t2, z2, g2, band, HB, H, spread_up(i3, 1), ROWS2 - 2, 2, 6)
    step = (own + 2) // 2
    for r0 in (0, step):
        lhs = jnp.concatenate(
            [
                g2[r0 + dr : r0 + dr + step, 1 - j % 2, (j + 1) // 2 : (j + 1) // 2 + ph].reshape(
                    step * ph * L, C2
                )
                for dr in range(3)
                for j in range(4)
            ],
            axis=1,
        )
        out = (dot_t(lhs, w2t[...]) * 0.25).reshape(step, ph, L, 2 * LANES)
        for u in range(2):
            i2[r0 : r0 + step, u] = out[..., u * LANES : (u + 1) * LANES]


def back1_body(dims, t1, z1, r1, i2, grad_ref, g1):
    H, L, HB, C1, C2, C3, C4, C5 = dims
    band = lax.axis_index("rows")
    ph = PH // 4

    def up(i0, chunk):
        v = i2[pl.ds(i0 // 2, chunk // 2 + 1)]
        v = jnp.stack([v[:, q % 2, q // 2] for q in range(2 * ph)], axis=1)
        return jnp.stack([v[(j + 1) // 2] for j in range(chunk)])

    pre_grads(1, t1, z1, g1, band, HB, H, up, ROWS1 - 1, 1, 6)
    lhs = jnp.concatenate(
        [g1[:, j].reshape((HB + 2) * L, LANES) for j in range(PH // 2 + 2)], axis=1
    )
    rows3 = dot_t(lhs, r1[...]).reshape(HB + 2, L, 2 * LANES)
    first = rows3[0:HB, :, 0:LANES].reshape(HB * L, LANES)
    second = rows3[1 : HB + 1, :, 0:LANES].reshape(HB * L, LANES)
    third = rows3[2 : HB + 2, :, LANES : 2 * LANES].reshape(HB * L, LANES)
    gin = (first + pltpu.roll(second, HALF, 1) + third)[:, 0:HALF]
    high = gin.astype(BF16)
    split = jnp.concatenate([high.astype(F32), gin - high.astype(F32)], axis=1).astype(BF16)
    width = PH * L
    sel_row = iota((LANES, width), 0) % HALF
    sel_col = iota((LANES, width), 1) % PH
    shape = (HB * L, width)
    inside = iota(shape, 1) // PH == iota(shape, 0) % L
    for ch in range(3):
        pick = jnp.where(sel_row == sel_col * 3 + ch, 1.0, 0.0).astype(BF16)
        wide = jnp.where(inside, dot(split, pick), 0.0)
        grad_ref[ch] = jnp.sum(wide.reshape(HB, L, width), axis=1)


ROWS1, ROWS2, ROWS3, ROWS4 = (8, 4, 4, 8)
TAP_ROWS = (6, 4, 4, 0, 0)
OTHER_ROWS = (4, 4, 4, 2, 1)
PAD = 2


def frame_work(x, c1, c2, b1, convs, biases, linears, HB):
    H, L, _ = x[0].shape
    H = H * len(x)
    C1, C2, C3, C4, C5 = [c.shape[-1] for c in convs]
    dims = (H, L, HB, C1, C2, C3, C4, C5)
    ph2, ph3, ph4 = (PH // 2, PH // 4, PH // 8)
    V = pltpu.VMEM
    far = [c.reshape(-1, c.shape[-1]) for c in convs[2:]]
    far += [v.reshape(1, -1) for v in (*biases[1:], *linears)]
    w1, r1, w2, w2t = call(
        weights_body,
        (
            V((4 * HALF, PH * HALF), BF16),
            V((4 * HALF, (ph2 + 2) * LANES), BF16),
            V((12 * C1, 2 * C2), BF16),
            V((4 * C1, 12 * C2), BF16),
        ),
        (c1, c2, b1),
        "weights",
        (V((3, HALF, LANES), F32), V((8, LANES), F32)),
        limit=8,
    )
    acts = (
        (HB + 3 * ROWS1, ph2, L, LANES),
        (HB // 2 + 3 * ROWS2, 2, ph3, L, C2),
        (HB // 4 + 3 * ROWS3, ph3, L, C3),
        (H // 8 + 4, ph4, L, C4),
        (H // 16 + 4, 1, L, C5),
    )
    outs = (V((8, LANES), F32),)
    halos = (1, 2, 2, 2, 2)
    outs += tuple(V(((HB >> i) + 2 * halos[i],) + s[1:], F32) for i, s in enumerate(acts))
    outs += tuple(V(s, F32) for s in acts)
    outs += tuple(V(v.shape, v.dtype) for v in far)
    loss, t1, t2, t3, t4, t5, z1, z2, z3, z4, z5, w3, w4, w5, *_ = call(
        functools.partial(forward_body, dims),
        outs,
        (*x, w1, w2),
        "forward",
        (
            V((H + 2, L, LANES), BF16),
            V((2, H, L, 2 * LANES), BF16),
            V((2, H // 2 + 2, ph2, L, LANES), BF16),
            V((2, H // 4 + 2, ph3 + 2, L, C2), BF16),
            V((2, H // 8 + 2, ph4 + 2, L, C3), BF16),
            V((2, H // 16 + 2, 3, L, C4), BF16),
            *[V((2, (H >> i) + 2 * PAD) + s[1:], BF16) for i, s in enumerate(acts)],
            pltpu.SemaphoreType.DMA((12,)),
        ),
        limit=32,
        far=far,
    )
    n1, n2, n3, n4, n5 = (HB + 2, HB // 2 + 4, HB // 4 + 4, HB // 8 + 4, HB // 16 + 4)

    def step(body, name, ins, out, scratch, flops):
        return call(functools.partial(body, dims), out, ins, name, (V(scratch, BF16),), 12, flops)

    def back5(_):
        return step(
            back5_body, "back5", (t5, z5, w5), V((n5 - 2, 1, L, C4), F32), (n5, 3, L, C5), FL
        )

    def back4(i5):
        return step(
            back4_body, "back4", (t4, z4, w4, i5), V((n4 - 2, ph4, L, C3), F32),
            (n4, ph4 + 2, L, C4), FL,
        )

    def back3(i4):
        return step(
            back3_body, "back3", (t3, z3, w3, i4), V((n3 - 2, ph3, L, C2), F32),
            (n3, ph3 + 2, L, C3), FL,
        )

    def back2(i3):
        return step(
            back2_body, "back2", (t2, z2, w2t, i3), V((n2 - 2, 2, ph3, L, LANES), F32),
            (n2, 2, ph3 + 2, L, C2), FL,
        )

    def back1(i2):
        return step(
            back1_body, "back1", (t1, z1, r1, i2),
            jax.ShapeDtypeStruct((3, HB, L * PH), F32), (n1, ph2 + 2, L, LANES), FL,
        )

    return loss, (back5, back4, back3, back2, back1)


FL = 10**9


def gather_bands(x):
    size = lax.axis_size("rows")
    assert size & (size - 1) == 0
    blocks = {0: x}
    hops = [h for h in (1 << k for k in range(size.bit_length() - 1))][::-1]
    for hop in hops:
        pairs = [(i, i ^ hop) for i in range(size)]
        for m in list(blocks):
            blocks[m ^ hop] = lax.ppermute(blocks[m], "rows", pairs)
    return [blocks[m] for m in range(size)]


def on_device(real_frames, fake_frames, *params):
    convs, biases, linears = (params[0:5], params[5:10], params[10:15])
    frames, _, band_rows, width = real_frames.shape
    bands = lax.axis_size("rows")
    frame_total = frames * lax.axis_size("dp")
    work = []
    for n in range(frames):
        c1, c2, b1 = (convs[0], convs[1], biases[0].reshape(1, -1))
        c2 = c2.reshape(9, *c2.shape[2:])
        x, c1, c2, b1 = prep(real_frames[n], fake_frames[n], c1, c2, b1)
        x = gather_bands(x)
        work.append(frame_work(x, c1, c2, b1, convs, biases, linears, band_rows))
    total = functools.reduce(jnp.add, [loss for loss, _ in work])
    hops = [("rows", 1)]
    size = lax.axis_size("dp")
    hops += [("dp", 1 << k) for k in range(size.bit_length() - 1)]
    assert size == 1 << len(hops) - 1
    states = [None] * frames
    done = 0
    for stage, (axis, hop) in enumerate(hops):
        pairs = [(i, i ^ hop) for i in range(lax.axis_size(axis))]
        other = lax.ppermute(total, axis, pairs)
        last = 5 if stage == len(hops) - 1 else (1, 3, 4)[min(stage, 2)]
        for k in range(done, last):
            states = [steps[k](s) for s, (_, steps) in zip(states, work)]
        done = last
        total, other, states = lax.optimization_barrier((total, other, states))
        total = total + other
    counts = [frame_total * (band_rows * bands >> s) * (width >> s) for s in range(5)]
    losses = jnp.sum(total, axis=1)[0:5] * jnp.array([1.0 / c for c in counts], F32)
    return (losses, jnp.stack(states))


def solution(mesh):
    frame = P("dp", None, "rows", None)
    return jax.shard_map(
        on_device,
        mesh=mesh,
        in_specs=(frame, frame) + (P(),) * 15,
        out_specs=(P(), frame),
        check_vma=False,
    )
```
